128 devices in a mesh: dp: 8 (over y_lo, z), head: 16 (over x, y_hi, core).
Axes of the slice: x: 4, y: 4 (y_hi: 2, y_lo: 2; y = y_hi * 2 + y_lo), z: 4, core: 2. Of those that a mesh axis runs over, the one named last changes fastest.
Arguments:
- projected: bfloat16 [49152, 24576], P(('dp', 'head')), may hold values from -64 to 64, as said below
- weight_exp: int32 [49152], P(('dp', 'head')), may hold values from 0 to 3
- damp_exp: int32 [128], replicated, may hold values from 0 to 2
Outputs:
- whitening: float32 [128, 192, 192], P('head')
The draws below stay inside these ranges and needn't reach their ends.
Inputs may be any that keep to these rules, and one draw needn't show every extreme that they name: `projected`: real values.
All inputs are finite; a program needn't handle non-finite values.
Results may differ from the reference program's by a relative error of at most 0.0003.
Values may be sent and summed in bfloat16 or wider, within the bound.
A program may use at most 192 MiB of HBM per device.

```python
import math
import jax
import jax.numpy as jnp
from jax import lax

HEADS = 64
HD = 192
TOKENS = 49152
MATS = 128


def draw_projected(key, part):
    first, second = jax.random.split(jax.random.fold_in(key, 11))
    base = jax.random.normal(first, (TOKENS, 2 * HEADS, HD), jnp.float32)
    scales = jnp.exp(jax.random.uniform(second, (2 * HEADS, HD), jnp.float32, 0.0, math.log(8.0)))
    mixed = base + 0.6 * jnp.roll(base, 1, axis=2) - 0.4 * jnp.roll(base, 5, axis=2)
    return jnp.clip((mixed * scales).reshape(TOKENS, 2 * HEADS * HD) / 4.0, -64.0, 64.0).astype(jnp.bfloat16)


def place_ends(entries, own_key, smallest, largest):
    longest = entries.shape.index(max(entries.shape))
    spots = []
    for shift in (0, 1):
        where = [jax.random.randint(jax.random.fold_in(own_key, axis), (), 0, length) for axis, length in enumerate(entries.shape)]
        where[longest] = (where[longest] + shift) % entries.shape[longest]
        spots.append(tuple(where))
    return entries.at[spots[0]].set(smallest).at[spots[1]].set(largest)


def setup_inputs(seed: int = 0) -> dict:
    seeds = jax.random.split(jax.random.key(seed), 4)
    return {
        "projected": draw_projected(jax.random.fold_in(seeds[3], 71), 0),
        "weight_exp": place_ends(jax.random.randint(seeds[1], (TOKENS,), 0, 4), jax.random.fold_in(seeds[1], 1), 0, 3).astype(jnp.int32),
        "damp_exp": place_ends(jax.random.randint(seeds[2], (MATS,), 0, 3), jax.random.fold_in(seeds[2], 1), 0, 2).astype(jnp.int32),
    }


def reference(projected, weight_exp, damp_exp):
    mats = projected.shape[1] // HD
    weights = jnp.exp2(weight_exp.astype(jnp.float32)).astype(jnp.bfloat16)
    scaled = projected * weights[:, None]
    eye = jnp.eye(HD, dtype=jnp.float32)

    def single(index):
        start = (index * HD).astype(jnp.int32)
        left = lax.dynamic_slice_in_dim(projected, start, HD, 1)
        right = lax.dynamic_slice_in_dim(scaled, start, HD, 1)
        gram = jnp.dot(left.T.astype(jnp.float32), right.astype(jnp.float32), preferred_element_type=jnp.float32) / TOKENS
        gram = 0.5 * (gram + gram.T)
        level = jnp.trace(gram) / HD + 1e-06
        damping = jnp.exp2(-damp_exp[index].astype(jnp.float32)) * level
        lower = jnp.linalg.cholesky(gram + damping * eye)
        return jax.scipy.linalg.solve_triangular(lower, eye, lower=True)
    return lax.map(single, jnp.arange(mats, dtype=jnp.int32))
```

```python
import functools
import jax
import jax.numpy as jnp
from jax import lax
from jax.experimental import pallas as pl
from jax.experimental.pallas import tpu as pltpu
from jax.sharding import PartitionSpec as P

HD = 192
ROWS = 56
MESH = pl.DeviceIdType.MESH
F32 = jnp.float32


def tdot(a, b):
    return lax.dot_general(a, b, (((0,), (0,)), ((), ())), preferred_element_type=F32)


def place():
    dp, head = lax.axis_index("dp"), lax.axis_index("head")
    x, y, z = head // 4, (head // 2) % 2 * 2 + dp // 4, dp % 4
    return x, y, z, head % 2


def device(x, y, z, core):
    return (y % 2 * 4 + z, x * 4 + y // 2 * 2 + core)


def rel(step):
    return (2 - step + (step // 2) * (7 - 2 * step)) % 4


def pack(low, high, put):
    r = lax.broadcasted_iota(jnp.int32, (128, 128), 0)
    c = lax.broadcasted_iota(jnp.int32, (128, 128), 1)
    odd = high[:, 128:]
    left = c < 64
    a = jnp.where(r >= c, low[:128, :128], odd)
    b = jnp.where(left, low[:128, 128:], high[:, :128])
    e = jnp.where(left[:64], low[128:192, 128:], low[192:, 128:])
    d = jnp.sum(jnp.where(r == c, odd, 0.0), axis=0, keepdims=True)
    put(0, 0, 0, a[:56])
    put(0, 1, 0, a[56:112])
    put(0, 2, 0, a[112:])
    put(0, 2, 16, b[:40])
    put(1, 0, 0, b[40:96])
    put(1, 1, 0, b[96:])
    put(1, 1, 32, e[:24])
    put(1, 2, 0, e[24:])
    put(1, 2, 40, jnp.broadcast_to(d, (16, 128)))


def dot(a, b, ca, cb):
    return lax.dot_general(a, b, (((ca,), (cb,)), ((), ())), precision=lax.Precision.HIGHEST,
                           preferred_element_type=F32)


def mul(a, b):
    return dot(a, b, 1, 0)


def mul_t(a, b):
    return dot(a, b, 1, 1)


def inverse_factor(d):
    r = lax.broadcasted_iota(jnp.int32, (64, 64), 0)
    c = lax.broadcasted_iota(jnp.int32, (64, 64), 1)
    full = jnp.concatenate([d, (r == c).astype(F32)], axis=1)
    m = [full[8 * i:8 * i + 8] for i in range(8)]
    sub = lax.broadcasted_iota(jnp.int32, (8, 128), 0)
    out = []

    def row(v, j):
        return jnp.broadcast_to(v[j:j + 1], (8, 128))

    for k in range(8):
        cs = {(i, j): jnp.broadcast_to(m[i][:, 8 * k + j:8 * k + j + 1], (8, 128))
              for i in range(k, 8) for j in range(8)}
        diag = jnp.ones((8, 128), F32)
        for j in range(8):
            pivot = row(cs[k, j], j)
            diag = jnp.where(sub == j, pivot, diag)
            inv = 1.0 / pivot
            scaled = row(m[k], j) * inv
            below = jnp.where(sub > j, cs[k, j], 0.0)
            us = {n: row(cs[k, n], j) * inv for n in range(j + 1, 8)}
            for i in range(k, 8):
                f = below if i == k else cs[i, j]
                m[i] = m[i] - f * scaled
                for n in range(j + 1, 8):
                    cs[i, n] = cs[i, n] - f * us[n]
        out.append((m[k] * lax.rsqrt(diag))[:, 64:])
    return jnp.concatenate(out, axis=0)


def whiten(flat, even, scale, total):
    r = lax.broadcasted_iota(jnp.int32, (128, 128), 0)
    c = lax.broadcasted_iota(jnp.int32, (128, 128), 1)
    flat = flat / total
    a, bc = flat[:128], flat[128:320]
    t = a.T
    low = jnp.where(r >= c, a, t)
    high = jnp.where(r < c, a, jnp.where(r == c, flat[320:321], t))
    a = jnp.where(even, low, high)
    b = jnp.where(even, bc[:, :64], bc[:, 64:])
    b0, b1, corner = b[:64], b[64:128], b[128:]
    a00, a10, a11 = a[:64, :64], a[64:, :64], a[64:, 64:]
    g00 = jnp.where(even, a00, corner)
    g10 = jnp.where(even, a10, b0)
    g11 = jnp.where(even, a11, a00)
    g20 = jnp.where(even, b0.T, b1)
    g21 = jnp.where(even, b1.T, a10)
    g22 = jnp.where(even, corner, a11)
    eye = r[:64, :64] == c[:64, :64]
    diag = jnp.where(eye, g00 + g11 + g22, 0.0)
    level = jnp.sum(jnp.sum(diag, axis=0, keepdims=True), axis=1, keepdims=True) / HD + 1e-06
    damp = jnp.where(eye, scale * level, 0.0)

    w00 = inverse_factor(g00 + damp)
    l10, l20 = mul_t(g10, w00), mul_t(g20, w00)
    s11 = g11 + damp - mul_t(l10, l10)
    s21 = g21 - mul_t(l20, l10)
    s22 = g22 + damp - mul_t(l20, l20)
    x10, x20 = mul(l10, w00), mul(l20, w00)
    w11 = inverse_factor(s11)
    l21 = mul_t(s21, w11)
    s22 = s22 - mul_t(l21, l21)
    w10 = -mul(w11, x10)
    x21 = mul(l21, w11)
    x20 = x20 + mul(l21, w10)
    w22 = inverse_factor(s22)
    return w00, w10, w11, -mul(w22, x20), -mul(w22, x21), w22


def whitening_kernel(total, x_ref, w_ref, damp_ref, out_ref, own, got, asem, bsem, xb, g, pr, rl, rr, fl, fr, f1, q2l, q2r, f2l, f2r, f2, f3, h,
                  xsem, dsend, drecv, rsem, ssem, fsem, s2send, q2sem, f2sem, s3send, s3sem, hsem):
    x, y, z, core = place()
    partner = device(x, y, z, 1 - core)
    right = (device((x + 1) % 4, y, z, core), device(x, (y + 1) % 4, z, core), device(x, y, (z + 1) % 4, core))
    left = (device((x + 3) % 4, y, z, core), device(x, (y + 3) % 4, z, core), device(x, y, (z + 3) % 4, core))
    far = (device((x + 2) % 4, y, z, core), device(x, (y + 2) % 4, z, core), device(x, y, (z + 2) % 4, core))

    def fetch(s, i):
        px = (x + rel(s // 2)) % 4
        py = (y + rel(s % 2 * 2 + i // 4)) % 4
        pz = (z + rel(i % 4)) % 4
        col = pl.multiple_of((px * 16 + py * 4 + pz) * 384, 384)
        return pltpu.make_async_copy(x_ref.at[:, pl.ds(col, 384)], xb.at[s % 2, i], xsem.at[s % 2, i])

    for i in range(8):
        fetch(0, i).start()

    barrier = pltpu.get_barrier_semaphore()
    base_y, low_y = y // 2 * 2, y % 2
    peers = [device(x, base_y + dy, (z + dz) % 4, cc) for dy in range(2) for dz in range(1, 4) for cc in range(2)]
    peers += [partner, device(x, base_y + 1 - low_y, z, 0), device(x, base_y + 1 - low_y, z, 1)]
    peers += [device((x + k) % 4, y, z, core) for k in range(1, 4)]
    peers += [device(x, (base_y + 2) % 4 + dy, z, core) for dy in range(2)]
    for peer in peers:
        pl.semaphore_signal(barrier, inc=1, device_id=peer, device_id_type=MESH)
    pl.semaphore_wait(barrier, len(peers))

    def remote(src, dst, send, recv, to):
        return pltpu.make_async_remote_copy(src_ref=src, dst_ref=dst, send_sem=send, recv_sem=recv,
                                            device_id=to, device_id_type=MESH)

    def halves(s):
        at = pl.ds(s * 8, 8)
        return remote(g.at[1 - core, :, at], pr.at[:, at], dsend, drecv.at[s], partner)

    def mine(col, first, count):
        return g.at[core, col, pl.ds(first, count)]

    def to_right(col, src, dst, sem):
        remote(src, dst, ssem.at[col, 0], sem, right[col]).start()

    def to_left(col, src, dst, sem):
        remote(src, dst, ssem.at[col, 1], sem, left[col]).start()

    def final_right(col, first, count, at):
        to_right(col, mine(col, first, count), fl.at[col, pl.ds(at, count)], fsem.at[col, 0])

    def final_left(col, first, count, at):
        to_left(col, mine(col, first, count), fr.at[col, pl.ds(at, count)], fsem.at[col, 1])

    def relay_right(col, first, count, at, sem):
        to_right(col, mine(col, first, count), rl.at[col, pl.ds(at, count)], rsem.at[0, sem])

    def relay_left(col, first, count, at, sem):
        to_left(col, mine(col, first, count), rr.at[col, pl.ds(at, count)], rsem.at[1, sem])

    def taken(buf, side, col, first, count, at, sem):
        part = buf.at[col, pl.ds(at, count)]
        remote(part, part, ssem.at[col, 0], rsem.at[side, sem], right[col]).wait_recv()
        g[core, col, pl.ds(first, count)] += buf[col, pl.ds(at, count)]

    def grams(s):
        for i in range(8):
            fetch(s, i).wait()

        w = w_ref[...]
        w3 = jnp.concatenate([w, w, w], axis=1)
        for i in range(8):
            t = xb[s % 2, i]
            tw = t * w3
            low = tdot(t[:, :256], tw[:, :256])
            high = tdot(t[:, 256:], tw[:, 128:])

            def put(half, col, row, value):
                g[half, col, s * 8 + i, pl.ds(row, value.shape[0]), :] = value

            pack(low, high, put)
        halves(s).start()

    def summed(s):
        base = s * 8
        halves(s).wait_recv()
        for col in range(3):
            g[core, col, pl.ds(base, 8)] += pr[col, pl.ds(base, 8)]
        xs, yh = s // 2, s % 2

        @pl.when(xs == 0)
        def _():
            relay_right(0, base, 4, yh * 4, yh)
            relay_left(0, base + 4, 4, yh * 4, yh)

        @pl.when(xs == 1)
        def _():
            final_right(0, base + 4, 4, yh * 8 + 4)

        @pl.when(xs == 2)
        def _():
            final_left(0, base, 4, yh * 8)

        @pl.when(yh == 0)
        def _():
            relay_right(1, base, 2, xs * 2, 2 + xs)
            relay_left(1, base + 2, 2, xs * 2, 2 + xs)
            final_right(1, base + 6, 2, xs * 4 + 2)

        @pl.when(yh == 1)
        def _():
            final_left(1, base, 2, xs * 4)

        relay_right(2, base, 1, s, 6 + s)
        relay_left(2, base + 4, 1, s, 6 + s)
        final_right(2, base + 5, 1, s * 2 + 1)
        final_left(2, base + 2, 1, s * 2)

    def passed(s):
        base = s * 8
        xs, yh = s // 2, s % 2

        @pl.when(xs == 1)
        def _():
            taken(rl, 0, 0, base, 4, yh * 4, yh)
            final_right(0, base, 4, yh * 8)

        @pl.when(xs == 2)
        def _():
            taken(rr, 1, 0, base + 4, 4, yh * 4, yh)
            final_left(0, base + 4, 4, yh * 8 + 4)

        @pl.when(yh == 0)
        def _():
            taken(rl, 0, 1, base + 4, 2, xs * 2, 2 + xs)
            final_right(1, base + 4, 2, xs * 4)

        @pl.when(yh == 1)
        def _():
            taken(rr, 1, 1, base + 2, 2, xs * 2, 2 + xs)
            final_left(1, base + 2, 2, xs * 4 + 2)

        taken(rl, 0, 2, base + 1, 1, s, 6 + s)
        final_right(2, base + 1, 1, s * 2)
        taken(rr, 1, 2, base + 6, 1, s, 6 + s)
        final_left(2, base + 6, 1, s * 2 + 1)

    def step(s, carry):
        @pl.when(s < 7)
        def _():
            for i in range(8):
                fetch(s + 1, i).start()

        grams(s)

        @pl.when(s >= 1)
        def _():
            summed(s - 1)

        @pl.when(s >= 2)
        def _():
            passed(s - 2)

        return carry

    lax.fori_loop(0, 8, step, 0)
    summed(7)
    passed(6)
    passed(7)

    axis2, axis3 = (1, 2, 0), (2, 0, 1)
    for col in range(3):
        for buf, side, to in ((fl, 0, left), (fr, 1, right)):
            remote(buf.at[col], buf.at[col], ssem.at[col, side], fsem.at[col, side], to[col]).wait_recv()
        for a in range(4):
            for b in range(4):
                slot = (48 + a * 4 + b, (2 * a + 1) * 8 + 4 + b, (2 * a + b // 2) * 8 + 3 + 4 * (b % 2))[col]
                at = b * 4 + a if col == 1 else a * 4 + b
                f1[col, at] = g[core, col, slot] + fl[col, a * 4 + b] + fr[col, a * 4 + b]
        ax = axis2[col]

        def part(first):
            return f1.at[col, pl.ds(first, 2)]

        remote(part(0), q2l.at[col], s2send.at[col, 0], q2sem.at[col, 0], right[ax]).start()
        remote(part(2), q2r.at[col], s2send.at[col, 1], q2sem.at[col, 1], left[ax]).start()
        remote(part(6), f2l.at[col, pl.ds(2, 2)], s2send.at[col, 0], f2sem.at[col, 0], right[ax]).start()
        remote(part(8), f2r.at[col, pl.ds(0, 2)], s2send.at[col, 1], f2sem.at[col, 1], left[ax]).start()
    for col in range(3):
        ax = axis2[col]
        remote(q2l.at[col], q2l.at[col], s2send.at[col, 0], q2sem.at[col, 0], right[ax]).wait_recv()
        f1[col, pl.ds(4, 2)] += q2l[col]
        remote(f1.at[col, pl.ds(4, 2)], f2l.at[col, pl.ds(0, 2)], s2send.at[col, 0], f2sem.at[col, 0], right[ax]).start()
        remote(q2r.at[col], q2r.at[col], s2send.at[col, 1], q2sem.at[col, 1], left[ax]).wait_recv()
        f1[col, pl.ds(10, 2)] += q2r[col]
        remote(f1.at[col, pl.ds(10, 2)], f2r.at[col, pl.ds(2, 2)], s2send.at[col, 1], f2sem.at[col, 1], left[ax]).start()
    for col in range(3):
        ax, ax3 = axis2[col], axis3[col]
        remote(f2l.at[col], f2l.at[col], s2send.at[col, 0], f2sem.at[col, 0], right[ax]).wait_recv()
        remote(f2r.at[col], f2r.at[col], s2send.at[col, 1], f2sem.at[col, 1], left[ax]).wait_recv()
        f2[col] = f1[col, pl.ds(12, 4)] + f2l[col] + f2r[col]
        for k, to in enumerate((far, right, left)):
            remote(f2.at[col, k], f3.at[col, k], s3send.at[col, k], s3sem.at[col, k], to[ax3]).start()
    for col in range(3):
        for k, to in enumerate((far, right, left)):
            remote(f2.at[col, k], f3.at[col, k], s3send.at[col, k], s3sem.at[col, k], to[axis3[col]]).wait_recv()
        h[core, col] = (f2[col, 3] + f3[col, 0]) + (f3[col, 1] + f3[col, 2])
    both = remote(h.at[core], h.at[core], hsem.at[0], hsem.at[1], partner)
    both.start()
    both.wait_recv()
    flat = jnp.concatenate([h[half, col] for half in range(2) for col in range(3)], axis=0)
    owner = (x * 16 + y * 4 + z) * 2 + core
    w00, w10, w11, w20, w21, w22 = whiten(flat, core == 0, damp_ref[owner], total)
    slot = z * 2 + core
    own[0:64] = jnp.concatenate([w00, w22], axis=1)
    own[64:128] = jnp.concatenate([w10, w11], axis=1)
    own[128:192] = jnp.concatenate([w20, w21], axis=1)

    def spread(k):
        to = device(x, base_y + (low_y + 1 - k // 4) % 2, (z + (2, 1, 3, 0)[k % 4]) % 4, low_y)
        return remote(own, got.at[slot], asem, bsem.at[slot], to)

    for k in range(7):
        spread(k).start()

    @pl.when(core != low_y)
    def _():
        spread(7).start()

    @pl.when(core == low_y)
    def _():
        got[slot] = own[...]

    for j in range(8):
        @pl.when(jnp.logical_or(core != low_y, slot != j))
        def _():
            remote(got.at[j], got.at[j], asem, bsem.at[j], partner).wait_recv()

        out_ref[j, 0:64, 0:64] = got[j, 0:64, 0:64]
        out_ref[j, 0:64, 64:192] = jnp.zeros((64, 128), F32)
        out_ref[j, 64:128, 0:128] = got[j, 64:128]
        out_ref[j, 64:128, 128:192] = jnp.zeros((64, 64), F32)
        out_ref[j, 128:192, 0:128] = got[j, 128:192]
        out_ref[j, 128:192, 128:192] = got[j, 0:64, 64:128]

    for col in range(3):
        for side in range(2):
            sent = g.at[core, col, pl.ds(0, 24)]
            remote(sent, sent, ssem.at[col, side], fsem.at[col, side], right[col]).wait_send()
            six = f1.at[col, pl.ds(0, 6)]
            remote(six, six, s2send.at[col, side], f2sem.at[col, side], right[col]).wait_send()
        for k in range(3):
            remote(f2.at[col, k], f3.at[col, k], s3send.at[col, k], s3sem.at[col, k], right[col]).wait_send()
    every = g.at[1 - core]
    remote(every, pr, dsend, drecv.at[0], partner).wait_send()
    both.wait_send()
    seven = got.at[pl.ds(0, 7)]
    remote(seven, seven, asem, bsem.at[0], partner).wait_send()

    @pl.when(core != low_y)
    def _():
        remote(got.at[0], got.at[0], asem, bsem.at[0], partner).wait_send()


def on_device(projected, weight_exp, damp_exp):
    weights = jnp.exp2(weight_exp.astype(F32)).astype(jnp.bfloat16)
    wide = jnp.broadcast_to(weights[:, None], (weights.shape[0], 128))
    scale = jnp.exp2(-damp_exp.astype(F32))
    total = projected.shape[0] * lax.axis_size('dp') * lax.axis_size('head')
    unit = (ROWS, 128)
    dma = pltpu.SemaphoreType.DMA
    return pl.pallas_call(
        functools.partial(whitening_kernel, total),
        out_shape=jax.ShapeDtypeStruct((8, HD, HD), F32),
        in_specs=[pl.BlockSpec(memory_space=pl.ANY), pl.BlockSpec(memory_space=pltpu.VMEM),
                  pl.BlockSpec(memory_space=pltpu.SMEM)],
        out_specs=pl.BlockSpec(memory_space=pltpu.VMEM),
        scratch_shapes=[
            pltpu.VMEM((HD, 128), F32), pltpu.VMEM((8, HD, 128), F32), dma, dma((8,)),
            pltpu.VMEM((2, 8, 384, 384), jnp.bfloat16),
            pltpu.VMEM((2, 3, 64) + unit, F32),
            pltpu.VMEM((3, 64) + unit, F32),
            pltpu.VMEM((3, 8) + unit, F32),
            pltpu.VMEM((3, 8) + unit, F32),
            pltpu.VMEM((3, 16) + unit, F32),
            pltpu.VMEM((3, 16) + unit, F32),
            pltpu.VMEM((3, 16) + unit, F32),
            pltpu.VMEM((3, 2) + unit, F32),
            pltpu.VMEM((3, 2) + unit, F32),
            pltpu.VMEM((3, 4) + unit, F32),
            pltpu.VMEM((3, 4) + unit, F32),
            pltpu.VMEM((3, 4) + unit, F32),
            pltpu.VMEM((3, 3) + unit, F32),
            pltpu.VMEM((2, 3) + unit, F32),
            dma((2, 8)), dma, dma((8,)), dma((2, 14)), dma((3, 2)), dma((3, 2)),
            dma((3, 2)), dma((3, 2)), dma((3, 2)), dma((3, 3)), dma((3, 3)), dma((2,)),
        ],
        compiler_params=pltpu.CompilerParams(collective_id=0, has_side_effects=True, vmem_limit_bytes=58 * 2**20),
        name="whitening",
    )(projected, wide, scale)


def solution(mesh):
    return jax.shard_map(
        on_device,
        mesh=mesh,
        in_specs=(P(("dp", "head"), None), P(("dp", "head")), P()),
        out_specs=P("head", None, None),
        check_vma=False,
    )
```

```python
import functools
import jax
import jax.numpy as jnp
from jax import lax
from jax.experimental import pallas as pl
from jax.experimental.pallas import tpu as pltpu
from jax.sharding import PartitionSpec as P

HD = 192
ROWS = 56
OUT = pltpu.VMEM
LAG = 8
MESH = pl.DeviceIdType.MESH
F32 = jnp.float32


def tdot(a, b):
    return lax.dot_general(a, b, (((0,), (0,)), ((), ())), preferred_element_type=F32)


def place():
    dp, head = lax.axis_index("dp"), lax.axis_index("head")
    x, y, z = head // 4, (head // 2) % 2 * 2 + dp // 4, dp % 4
    return x, y, z, head % 2


def device(x, y, z, core):
    return (y % 2 * 4 + z, x * 4 + y // 2 * 2 + core)


def rel(step):
    return (2 - step + (step // 2) * (7 - 2 * step)) % 4


def pack(low, high, put):
    r = lax.broadcasted_iota(jnp.int32, (128, 128), 0)
    c = lax.broadcasted_iota(jnp.int32, (128, 128), 1)
    odd = high[:, 128:]
    left = c < 64
    a = jnp.where(r >= c, low[:128, :128], odd)
    b = jnp.where(left, low[:128, 128:], high[:, :128])
    e = jnp.where(left[:64], low[128:192, 128:], low[192:, 128:])
    d = jnp.sum(jnp.where(r == c, odd, 0.0), axis=0, keepdims=True)
    put(0, 0, 0, a[:56])
    put(0, 1, 0, a[56:112])
    put(0, 2, 0, a[112:])
    put(0, 2, 16, b[:40])
    put(1, 0, 0, b[40:96])
    put(1, 1, 0, b[96:])
    put(1, 1, 32, e[:24])
    put(1, 2, 0, e[24:])
    put(1, 2, 40, jnp.broadcast_to(d, (16, 128)))


def dot(a, b, ca, cb):
    return lax.dot_general(a, b, (((ca,), (cb,)), ((), ())), precision=lax.Precision.HIGHEST,
                           preferred_element_type=F32)


def mul(a, b):
    return dot(a, b, 1, 0)


def mul_t(a, b):
    return dot(a, b, 1, 1)


def inverse_factor(d):
    r = lax.broadcasted_iota(jnp.int32, (64, 64), 0)
    c = lax.broadcasted_iota(jnp.int32, (64, 64), 1)
    full = jnp.concatenate([d, (r == c).astype(F32)], axis=1)
    m = [full[8 * i:8 * i + 8] for i in range(8)]
    sub = lax.broadcasted_iota(jnp.int32, (8, 128), 0)
    out = []

    def row(v, j):
        return jnp.broadcast_to(v[j:j + 1], (8, 128))

    for k in range(8):
        cs = {(i, j): jnp.broadcast_to(m[i][:, 8 * k + j:8 * k + j + 1], (8, 128))
              for i in range(k, 8) for j in range(8)}
        diag = jnp.ones((8, 128), F32)
        for j in range(8):
            pivot = row(cs[k, j], j)
            diag = jnp.where(sub == j, pivot, diag)
            inv = 1.0 / pivot
            scaled = row(m[k], j) * inv
            below = jnp.where(sub > j, cs[k, j], 0.0)
            us = {n: row(cs[k, n], j) * inv for n in range(j + 1, 8)}
            for i in range(k, 8):
                f = below if i == k else cs[i, j]
                m[i] = m[i] - f * scaled
                for n in range(j + 1, 8):
                    cs[i, n] = cs[i, n] - f * us[n]
        out.append((m[k] * lax.rsqrt(diag))[:, 64:])
    return jnp.concatenate(out, axis=0)


def folded(a):
    return jnp.concatenate([a[:32], a[32:]], axis=1)


def whiten(flat, even, scale, total, emit):
    r = lax.broadcasted_iota(jnp.int32, (128, 128), 0)
    c = lax.broadcasted_iota(jnp.int32, (128, 128), 1)
    flat = flat / total
    a, bc = flat[:128], flat[128:320]
    t = a.T
    low = jnp.where(r >= c, a, t)
    high = jnp.where(r < c, a, jnp.where(r == c, flat[320:321], t))
    a = jnp.where(even, low, high)
    b = jnp.where(even, bc[:, :64], bc[:, 64:])
    b0, b1, corner = b[:64], b[64:128], b[128:]
    a00, a10, a11 = a[:64, :64], a[64:, :64], a[64:, 64:]
    g00 = jnp.where(even, a00, corner)
    g10 = jnp.where(even, a10, b0)
    g11 = jnp.where(even, a11, a00)
    g20 = jnp.where(even, b0.T, b1)
    g21 = jnp.where(even, b1.T, a10)
    g22 = jnp.where(even, corner, a11)
    eye = r[:64, :64] == c[:64, :64]
    diag = jnp.where(eye, g00 + g11 + g22, 0.0)
    level = jnp.sum(jnp.sum(diag, axis=0, keepdims=True), axis=1, keepdims=True) / HD + 1e-06
    damp = jnp.where(eye, scale * level, 0.0)

    w00 = inverse_factor(g00 + damp)
    emit(0, 32, folded(w00))
    l10, l20 = mul_t(g10, w00), mul_t(g20, w00)
    s11 = g11 + damp - mul_t(l10, l10)
    s21 = g21 - mul_t(l20, l10)
    s22 = g22 + damp - mul_t(l20, l20)
    x10, x20 = mul(l10, w00), mul(l20, w00)
    w11 = inverse_factor(s11)
    l21 = mul_t(s21, w11)
    s22 = s22 - mul_t(l21, l21)
    w10 = -mul(w11, x10)
    emit(32, 64, jnp.concatenate([w10, w11], axis=1))
    x21 = mul(l21, w11)
    x20 = x20 + mul(l21, w10)
    w22 = inverse_factor(s22)
    last = jnp.concatenate([-mul(w22, x20), -mul(w22, x21)], axis=1)
    emit(96, 96, jnp.concatenate([last, folded(w22)], axis=0))


def whitening_kernel(total, x_ref, weight_ref, damp_ref, got, wexp, dexp, w_ref, esem, own, asem, bsem, xb, g, pr, rl, rr, fl, fr, f1, q2l, q2r, f2l, f2r, f2, f3, h,
                  xsem, dsend, drecv, rsem, ssem, fsem, s2send, q2sem, f2sem, s3send, s3sem, hsem):
    x, y, z, core = place()
    partner = device(x, y, z, 1 - core)
    right = (device((x + 1) % 4, y, z, core), device(x, (y + 1) % 4, z, core), device(x, y, (z + 1) % 4, core))
    left = (device((x + 3) % 4, y, z, core), device(x, (y + 3) % 4, z, core), device(x, y, (z + 3) % 4, core))
    far = (device((x + 2) % 4, y, z, core), device(x, (y + 2) % 4, z, core), device(x, y, (z + 2) % 4, core))

    def fetch(s, i):
        px = (x + rel(s // 2)) % 4
        py = (y + rel(s % 2 * 2 + i // 4)) % 4
        pz = (z + rel(i % 4)) % 4
        col = pl.multiple_of((px * 16 + py * 4 + pz) * 384, 384)
        return pltpu.make_async_copy(x_ref.at[:, pl.ds(col, 384)], xb.at[s % 2, i], xsem.at[s % 2, i])

    for i in range(8):
        fetch(0, i).start()

    exps = (pltpu.make_async_copy(weight_ref, wexp, esem.at[0]), pltpu.make_async_copy(damp_ref, dexp, esem.at[1]))
    for copy in exps:
        copy.start()

    barrier = pltpu.get_barrier_semaphore()
    base_y, low_y = y // 2 * 2, y % 2
    peers = [device(x, base_y + dy, (z + dz) % 4, cc) for dy in range(2) for dz in range(1, 4) for cc in range(2)]
    peers += [partner, device(x, base_y + 1 - low_y, z, 0), device(x, base_y + 1 - low_y, z, 1)]
    peers += [device((x + k) % 4, y, z, core) for k in range(1, 4)]
    peers += [device(x, (base_y + 2) % 4 + dy, z, core) for dy in range(2)]
    for peer in peers:
        pl.semaphore_signal(barrier, inc=1, device_id=peer, device_id_type=MESH)
    for copy in exps:
        copy.wait()
    for k in range(3):
        line = jnp.exp2(wexp[pl.ds(128 * k, 128)].astype(F32)).reshape(1, 128)
        w_ref[pl.ds(128 * k, 128)] = jnp.broadcast_to(line, (128, 128)).T.astype(jnp.bfloat16)

    def remote(src, dst, send, recv, to):
        return pltpu.make_async_remote_copy(src_ref=src, dst_ref=dst, send_sem=send, recv_sem=recv,
                                            device_id=to, device_id_type=MESH)

    def halves(s):
        at = pl.ds(s * 8, 8)
        return remote(g.at[1 - core, :, at], pr.at[:, at], dsend, drecv.at[s], partner)

    def mine(col, first, count):
        return g.at[core, col, pl.ds(first, count)]

    def to_right(col, src, dst, sem):
        remote(src, dst, ssem.at[col, 0], sem, right[col]).start()

    def to_left(col, src, dst, sem):
        remote(src, dst, ssem.at[col, 1], sem, left[col]).start()

    def final_right(col, first, count, at):
        to_right(col, mine(col, first, count), fl.at[col, pl.ds(at, count)], fsem.at[col, 0])

    def final_left(col, first, count, at):
        to_left(col, mine(col, first, count), fr.at[col, pl.ds(at, count)], fsem.at[col, 1])

    def relay_right(col, first, count, at, sem):
        to_right(col, mine(col, first, count), rl.at[col, pl.ds(at, count)], rsem.at[0, sem])

    def relay_left(col, first, count, at, sem):
        to_left(col, mine(col, first, count), rr.at[col, pl.ds(at, count)], rsem.at[1, sem])

    def taken(buf, side, col, first, count, at, sem):
        part = buf.at[col, pl.ds(at, count)]
        remote(part, part, ssem.at[col, 0], rsem.at[side, sem], right[col]).wait_recv()
        g[core, col, pl.ds(first, count)] += buf[col, pl.ds(at, count)]

    def grams(s):
        for i in range(8):
            fetch(s, i).wait()

        w = w_ref[...]
        w3 = jnp.concatenate([w, w, w], axis=1)
        for i in range(8):
            t = xb[s % 2, i]
            tw = t * w3
            low = tdot(t[:, :256], tw[:, :256])
            high = tdot(t[:, 256:], tw[:, 128:])

            def put(half, col, row, value):
                g[half, col, s * 8 + i, pl.ds(row, value.shape[0]), :] = value

            pack(low, high, put)

        @pl.when(s == 0)
        def _():
            pl.semaphore_wait(barrier, len(peers))

        halves(s).start()

    def summed(s):
        base = s * 8
        halves(s).wait_recv()
        for col in range(3):
            g[core, col, pl.ds(base, 8)] += pr[col, pl.ds(base, 8)]
        xs, yh = s // 2, s % 2

        @pl.when(xs == 0)
        def _():
            relay_right(0, base, 4, yh * 4, yh)
            relay_left(0, base + 4, 4, yh * 4, yh)

        @pl.when(xs == 1)
        def _():
            final_right(0, base + 4, 4, yh * 8 + 4)

        @pl.when(xs == 2)
        def _():
            final_left(0, base, 4, yh * 8)

        @pl.when(yh == 0)
        def _():
            relay_right(1, base, 2, xs * 2, 2 + xs)
            relay_left(1, base + 2, 2, xs * 2, 2 + xs)
            final_right(1, base + 6, 2, xs * 4 + 2)

        @pl.when(yh == 1)
        def _():
            final_left(1, base, 2, xs * 4)

        relay_right(2, base, 1, s, 6 + s)
        relay_left(2, base + 4, 1, s, 6 + s)
        final_right(2, base + 5, 1, s * 2 + 1)
        final_left(2, base + 2, 1, s * 2)

    def passed(s):
        base = s * 8
        xs, yh = s // 2, s % 2

        @pl.when(xs == 1)
        def _():
            taken(rl, 0, 0, base, 4, yh * 4, yh)
            final_right(0, base, 4, yh * 8)

        @pl.when(xs == 2)
        def _():
            taken(rr, 1, 0, base + 4, 4, yh * 4, yh)
            final_left(0, base + 4, 4, yh * 8 + 4)

        @pl.when(yh == 0)
        def _():
            taken(rl, 0, 1, base + 4, 2, xs * 2, 2 + xs)
            final_right(1, base + 4, 2, xs * 4)

        @pl.when(yh == 1)
        def _():
            taken(rr, 1, 1, base + 2, 2, xs * 2, 2 + xs)
            final_left(1, base + 2, 2, xs * 4 + 2)

        taken(rl, 0, 2, base + 1, 1, s, 6 + s)
        final_right(2, base + 1, 1, s * 2)
        taken(rr, 1, 2, base + 6, 1, s, 6 + s)
        final_left(2, base + 6, 1, s * 2 + 1)

    def step(s, carry):
        @pl.when(s < 7)
        def _():
            for i in range(8):
                fetch(s + 1, i).start()

        grams(s)

        @pl.when(s >= 1)
        def _():
            summed(s - 1)

        @pl.when(s >= LAG)
        def _():
            passed(s - LAG)

        return carry

    lax.fori_loop(0, 8, step, 0)
    summed(7)

    def rest(s, carry):
        passed(s)
        return carry

    lax.fori_loop(8 - LAG, 8, rest, 0)

    axis2, axis3 = (1, 2, 0), (2, 0, 1)
    for col in range(3):
        for buf, side, to in ((fl, 0, left), (fr, 1, right)):
            remote(buf.at[col], buf.at[col], ssem.at[col, side], fsem.at[col, side], to[col]).wait_recv()
        for a in range(4):
            for b in range(4):
                slot = (48 + a * 4 + b, (2 * a + 1) * 8 + 4 + b, (2 * a + b // 2) * 8 + 3 + 4 * (b % 2))[col]
                at = b * 4 + a if col == 1 else a * 4 + b
                f1[col, at] = g[core, col, slot] + fl[col, a * 4 + b] + fr[col, a * 4 + b]
        ax = axis2[col]

        def part(first):
            return f1.at[col, pl.ds(first, 2)]

        remote(part(0), q2l.at[col], s2send.at[col, 0], q2sem.at[col, 0], right[ax]).start()
        remote(part(2), q2r.at[col], s2send.at[col, 1], q2sem.at[col, 1], left[ax]).start()
        remote(part(6), f2l.at[col, pl.ds(2, 2)], s2send.at[col, 0], f2sem.at[col, 0], right[ax]).start()
        remote(part(8), f2r.at[col, pl.ds(0, 2)], s2send.at[col, 1], f2sem.at[col, 1], left[ax]).start()
    for col in range(3):
        ax = axis2[col]
        remote(q2l.at[col], q2l.at[col], s2send.at[col, 0], q2sem.at[col, 0], right[ax]).wait_recv()
        f1[col, pl.ds(4, 2)] += q2l[col]
        remote(f1.at[col, pl.ds(4, 2)], f2l.at[col, pl.ds(0, 2)], s2send.at[col, 0], f2sem.at[col, 0], right[ax]).start()
        remote(q2r.at[col], q2r.at[col], s2send.at[col, 1], q2sem.at[col, 1], left[ax]).wait_recv()
        f1[col, pl.ds(10, 2)] += q2r[col]
        remote(f1.at[col, pl.ds(10, 2)], f2r.at[col, pl.ds(2, 2)], s2send.at[col, 1], f2sem.at[col, 1], left[ax]).start()
    for col in range(3):
        ax, ax3 = axis2[col], axis3[col]
        remote(f2l.at[col], f2l.at[col], s2send.at[col, 0], f2sem.at[col, 0], right[ax]).wait_recv()
        remote(f2r.at[col], f2r.at[col], s2send.at[col, 1], f2sem.at[col, 1], left[ax]).wait_recv()
        f2[col] = f1[col, pl.ds(12, 4)] + f2l[col] + f2r[col]
        for k, to in enumerate((far, right, left)):
            remote(f2.at[col, k], f3.at[col, k], s3send.at[col, k], s3sem.at[col, k], to[ax3]).start()
    for col in range(3):
        for k, to in enumerate((far, right, left)):
            remote(f2.at[col, k], f3.at[col, k], s3send.at[col, k], s3sem.at[col, k], to[axis3[col]]).wait_recv()
        h[core, col] = (f2[col, 3] + f3[col, 0]) + (f3[col, 1] + f3[col, 2])
    both = remote(h.at[core], h.at[core], hsem.at[0], hsem.at[1], partner)
    both.start()
    both.wait_recv()
    flat = jnp.concatenate([h[half, col] for half in range(2) for col in range(3)], axis=0)
    owner = (x * 16 + y * 4 + z) * 2 + core
    lane = lax.broadcasted_iota(jnp.int32, (1, 128), 1)
    exponent = jnp.where(lane == owner, dexp[...].astype(F32).reshape(1, 128), 0.0)
    scale = jnp.exp2(-jnp.sum(exponent, axis=1, keepdims=True))
    slot = z * 2 + core

    def emit(first, count, value):
        rows = pl.ds(first, count)
        own[rows] = value
        for k in range(8):
            to = device(x, base_y + (low_y + 1 - k // 4) % 2, (z + (2, 1, 3, 0)[k % 4]) % 4, low_y)
            copy = remote(own.at[rows], got.at[slot, rows], asem, bsem.at[slot], to)
            if k < 7:
                copy.start()
            else:
                pl.when(core != low_y)(copy.start)

        @pl.when(core == low_y)
        def _():
            got[slot, rows] = value

    whiten(flat, core == 0, scale, total, emit)

    for j in range(8):
        @pl.when(jnp.logical_or(core != low_y, slot != j))
        def _():
            remote(got.at[j], got.at[j], asem, bsem.at[j], partner).wait_recv()

    for col in range(3):
        for side in range(2):
            sent = g.at[core, col, pl.ds(0, 24)]
            remote(sent, sent, ssem.at[col, side], fsem.at[col, side], right[col]).wait_send()
            six = f1.at[col, pl.ds(0, 6)]
            remote(six, six, s2send.at[col, side], f2sem.at[col, side], right[col]).wait_send()
        for k in range(3):
            remote(f2.at[col, k], f3.at[col, k], s3send.at[col, k], s3sem.at[col, k], right[col]).wait_send()
    every = g.at[1 - core]
    remote(every, pr, dsend, drecv.at[0], partner).wait_send()
    both.wait_send()
    seven = got.at[pl.ds(0, 7)]
    remote(seven, seven, asem, bsem.at[0], partner).wait_send()

    @pl.when(core != low_y)
    def _():
        remote(got.at[0], got.at[0], asem, bsem.at[0], partner).wait_send()


def unpack_kernel(packed, out_ref, full, sem):
    copies = []
    for j in range(8):
        full[j, 0:32, 0:64] = packed[j, 0:32, 0:64]
        full[j, 32:64, 0:64] = packed[j, 0:32, 64:128]
        full[j, 0:64, 64:192] = jnp.zeros((64, 128), F32)
        full[j, 64:128, 0:128] = packed[j, 32:96]
        full[j, 64:128, 128:192] = jnp.zeros((64, 64), F32)
        full[j, 128:192, 0:128] = packed[j, 96:160]
        full[j, 128:160, 128:192] = packed[j, 160:192, 0:64]
        full[j, 160:192, 128:192] = packed[j, 160:192, 64:128]
        copies.append(pltpu.make_async_copy(full.at[j], out_ref.at[j], sem.at[j]))
        copies[-1].start()
    for copy in copies:
        copy.wait()


def on_device(projected, weight_exp, damp_exp):
    total = projected.shape[0] * lax.axis_size('dp') * lax.axis_size('head')
    unit = (ROWS, 128)
    dma = pltpu.SemaphoreType.DMA
    packed = pl.pallas_call(
        functools.partial(whitening_kernel, total),
        out_shape=OUT((8, HD, 128), F32),
        in_specs=[pl.BlockSpec(memory_space=pl.ANY), pl.BlockSpec(memory_space=pl.ANY),
                  pl.BlockSpec(memory_space=pl.ANY)],
        out_specs=pl.BlockSpec(memory_space=pltpu.VMEM),
        scratch_shapes=[
            pltpu.VMEM((384,), jnp.int32), pltpu.VMEM((128,), jnp.int32), pltpu.VMEM((384, 128), jnp.bfloat16), dma((2,)),
            pltpu.VMEM((HD, 128), F32), dma, dma((8,)),
            pltpu.VMEM((2, 8, 384, 384), jnp.bfloat16),
            pltpu.VMEM((2, 3, 64) + unit, F32),
            pltpu.VMEM((3, 64) + unit, F32),
            pltpu.VMEM((3, 8) + unit, F32),
            pltpu.VMEM((3, 8) + unit, F32),
            pltpu.VMEM((3, 16) + unit, F32),
            pltpu.VMEM((3, 16) + unit, F32),
            pltpu.VMEM((3, 16) + unit, F32),
            pltpu.VMEM((3, 2) + unit, F32),
            pltpu.VMEM((3, 2) + unit, F32),
            pltpu.VMEM((3, 4) + unit, F32),
            pltpu.VMEM((3, 4) + unit, F32),
            pltpu.VMEM((3, 4) + unit, F32),
            pltpu.VMEM((3, 3) + unit, F32),
            pltpu.VMEM((2, 3) + unit, F32),
            dma((2, 8)), dma, dma((8,)), dma((2, 14)), dma((3, 2)), dma((3, 2)),
            dma((3, 2)), dma((3, 2)), dma((3, 2)), dma((3, 3)), dma((3, 3)), dma((2,)),
        ],
        compiler_params=pltpu.CompilerParams(collective_id=0, has_side_effects=True, vmem_limit_bytes=58 * 2**20),
        name="whitening",
    )(projected, weight_exp, damp_exp)
    return pl.pallas_call(
        unpack_kernel,
        out_shape=jax.ShapeDtypeStruct((8, HD, HD), F32),
        in_specs=[pl.BlockSpec(memory_space=pltpu.VMEM)],
        out_specs=pl.BlockSpec(memory_space=pl.ANY),
        scratch_shapes=[pltpu.VMEM((8, HD, HD), F32), dma((8,))],
        name="unpack",
    )(pltpu.with_memory_space_constraint(packed, pltpu.VMEM))


def solution(mesh):
    return jax.shard_map(
        on_device,
        mesh=mesh,
        in_specs=(P(("dp", "head"), None), P(("dp", "head")), P()),
        out_specs=P("head", None, None),
        check_vma=False,
    )
```

```python
import functools
import jax
import jax.numpy as jnp
from jax import lax
from jax.experimental import pallas as pl
from jax.experimental.pallas import tpu as pltpu
from jax.sharding import PartitionSpec as P

HD = 192
ROWS = 56
OUT = pltpu.VMEM
LAG = 4
LAG_X = 3
MESH = pl.DeviceIdType.MESH
F32 = jnp.float32


def tdot(a, b):
    return lax.dot_general(a, b, (((0,), (0,)), ((), ())), preferred_element_type=F32)


def place():
    dp, head = lax.axis_index("dp"), lax.axis_index("head")
    x, y, z = head // 4, (head // 2) % 2 * 2 + dp // 4, dp % 4
    return x, y, z, head % 2


def device(x, y, z, core):
    return (y % 2 * 4 + z, x * 4 + y // 2 * 2 + core)


GROUPS = ((0, 0), (1, 0), (0, 1), (2, 0), (1, 1), (3, 0), (2, 1), (3, 1))


def order(s):
    xs = sum(x << (2 * i) for i, (x, _) in enumerate(GROUPS))
    ys = sum(y << i for i, (_, y) in enumerate(GROUPS))
    return lax.shift_right_logical(jnp.int32(xs), jnp.int32(2 * s)) % 4, lax.shift_right_logical(jnp.int32(ys), jnp.int32(s)) % 2


def rel(step):
    return (2 - step + (step // 2) * (7 - 2 * step)) % 4


def pack(low, high, put):
    r = lax.broadcasted_iota(jnp.int32, (128, 128), 0)
    c = lax.broadcasted_iota(jnp.int32, (128, 128), 1)
    odd = high[:, 128:]
    left = c < 64
    a = jnp.where(r >= c, low[:128, :128], odd)
    b = jnp.where(left, low[:128, 128:], high[:, :128])
    e = jnp.where(left[:64], low[128:192, 128:], low[192:, 128:])
    d = jnp.sum(jnp.where(r == c, odd, 0.0), axis=0, keepdims=True)
    put(0, 0, 0, a[:56])
    put(0, 1, 0, a[56:112])
    put(0, 2, 0, a[112:])
    put(0, 2, 16, b[:40])
    put(1, 0, 0, b[40:96])
    put(1, 1, 0, b[96:])
    put(1, 1, 32, e[:24])
    put(1, 2, 0, e[24:])
    put(1, 2, 40, jnp.broadcast_to(d, (16, 128)))


def dot(a, b, ca, cb):
    return lax.dot_general(a, b, (((ca,), (cb,)), ((), ())), precision=lax.Precision.HIGHEST,
                           preferred_element_type=F32)


def mul(a, b):
    return dot(a, b, 1, 0)


def mul_t(a, b):
    return dot(a, b, 1, 1)


def inverse_factor(d):
    r = lax.broadcasted_iota(jnp.int32, (64, 64), 0)
    c = lax.broadcasted_iota(jnp.int32, (64, 64), 1)
    full = jnp.concatenate([d, (r == c).astype(F32)], axis=1)
    m = [full[8 * i:8 * i + 8] for i in range(8)]
    sub = lax.broadcasted_iota(jnp.int32, (8, 128), 0)
    out = []

    def row(v, j):
        return jnp.broadcast_to(v[j:j + 1], (8, 128))

    for k in range(8):
        cs = {(i, j): jnp.broadcast_to(m[i][:, 8 * k + j:8 * k + j + 1], (8, 128))
              for i in range(k, 8) for j in range(8)}
        diag = jnp.ones((8, 128), F32)
        for j in range(0, 8, 2):
            a, b, e = row(cs[k, j], j), row(cs[k, j + 1], j), row(cs[k, j + 1], j + 1)
            det = a * e - b * b
            inv, over = 1.0 / det, 1.0 / a
            ei, bi, ai = e * inv, b * inv, a * inv
            r0, r1 = row(m[k], j), row(m[k], j + 1)
            t0, t1 = ei * r0 - bi * r1, ai * r1 - bi * r0
            below = sub > j + 1
            second = jnp.where(sub == j + 1, b * over * r0, 0.0)
            diag = jnp.where(sub == j, a, jnp.where(sub == j + 1, det * over, diag))
            us = {}
            for n in range(j + 2, 8):
                c0, c1 = row(cs[k, n], j), row(cs[k, n], j + 1)
                us[n] = (ei * c0 - bi * c1, ai * c1 - bi * c0)
            for i in range(k, 8):
                f0, f1 = cs[i, j], cs[i, j + 1]
                if i == k:
                    f0, f1 = jnp.where(below, f0, 0.0), jnp.where(below, f1, 0.0)
                    m[i] = m[i] - (f0 * t0 + f1 * t1 + second)
                else:
                    m[i] = m[i] - (f0 * t0 + f1 * t1)
                for n in range(j + 2, 8):
                    cs[i, n] = cs[i, n] - (f0 * us[n][0] + f1 * us[n][1])
        out.append((m[k] * lax.rsqrt(diag))[:, 64:])
    return jnp.concatenate(out, axis=0)


def folded(a):
    return jnp.concatenate([a[:32], a[32:]], axis=1)


def whiten(flat, even, scale, total, emit):
    r = lax.broadcasted_iota(jnp.int32, (128, 128), 0)
    c = lax.broadcasted_iota(jnp.int32, (128, 128), 1)
    flat = flat / total
    a, bc = flat[:128], flat[128:320]
    t = a.T
    low = jnp.where(r >= c, a, t)
    high = jnp.where(r < c, a, jnp.where(r == c, flat[320:321], t))
    a = jnp.where(even, low, high)
    b = jnp.where(even, bc[:, :64], bc[:, 64:])
    b0, b1, corner = b[:64], b[64:128], b[128:]
    a00, a10, a11 = a[:64, :64], a[64:, :64], a[64:, 64:]
    g00 = jnp.where(even, a00, corner)
    g10 = jnp.where(even, a10, b0)
    g11 = jnp.where(even, a11, a00)
    g20 = jnp.where(even, b0.T, b1)
    g21 = jnp.where(even, b1.T, a10)
    g22 = jnp.where(even, corner, a11)
    eye = r[:64, :64] == c[:64, :64]
    diag = jnp.where(eye, g00 + g11 + g22, 0.0)
    level = jnp.sum(jnp.sum(diag, axis=0, keepdims=True), axis=1, keepdims=True) / HD + 1e-06
    damp = jnp.where(eye, scale * level, 0.0)

    w00 = inverse_factor(g00 + damp)
    emit(0, 32, folded(w00))
    l10, l20 = mul_t(g10, w00), mul_t(g20, w00)
    s11 = g11 + damp - mul_t(l10, l10)
    s21 = g21 - mul_t(l20, l10)
    s22 = g22 + damp - mul_t(l20, l20)
    x10, x20 = mul(l10, w00), mul(l20, w00)
    w11 = inverse_factor(s11)
    l21 = mul_t(s21, w11)
    s22 = s22 - mul_t(l21, l21)
    w10 = -mul(w11, x10)
    emit(32, 64, jnp.concatenate([w10, w11], axis=1))
    x21 = mul(l21, w11)
    x20 = x20 + mul(l21, w10)
    w22 = inverse_factor(s22)
    last = jnp.concatenate([-mul(w22, x20), -mul(w22, x21)], axis=1)
    emit(96, 96, jnp.concatenate([last, folded(w22)], axis=0))


def whitening_kernel(total, x_ref, weight_ref, damp_ref, got, wexp, dexp, w_ref, esem, own, asem, bsem, xb, g, pr, rl, rr, fl, fr, f1, q2, f2, f3, h,
                  xsem, dsend, drecv, rsem, ssem, fsem, s2send, q2sem, s3send, s3sem, hsem):
    x, y, z, core = place()
    partner = device(x, y, z, 1 - core)
    right = (device((x + 1) % 4, y, z, core), device(x, (y + 1) % 4, z, core), device(x, y, (z + 1) % 4, core))
    left = (device((x + 3) % 4, y, z, core), device(x, (y + 3) % 4, z, core), device(x, y, (z + 3) % 4, core))
    far = (device((x + 2) % 4, y, z, core), device(x, (y + 2) % 4, z, core), device(x, y, (z + 2) % 4, core))

    def fetch(s, i):
        xs, yh = order(s)
        px = (x + rel(xs)) % 4
        py = (y + rel(yh * 2 + i // 4)) % 4
        pz = (z + rel(i % 4)) % 4
        col = pl.multiple_of((px * 16 + py * 4 + pz) * 384, 384)
        return pltpu.make_async_copy(x_ref.at[:, pl.ds(col, 384)], xb.at[s % 2, i], xsem.at[s % 2, i])

    for i in range(8):
        fetch(0, i).start()

    exps = (pltpu.make_async_copy(weight_ref, wexp, esem.at[0]), pltpu.make_async_copy(damp_ref, dexp, esem.at[1]))
    for copy in exps:
        copy.start()

    barrier = pltpu.get_barrier_semaphore()
    base_y, low_y = y // 2 * 2, y % 2
    peers = [device(x, base_y + dy, (z + dz) % 4, cc) for dy in range(2) for dz in range(1, 4) for cc in range(2)]
    peers += [partner, device(x, base_y + 1 - low_y, z, 0), device(x, base_y + 1 - low_y, z, 1)]
    peers += [device((x + k) % 4, y, z, core) for k in range(1, 4)]
    peers += [device(x, (base_y + 2) % 4 + dy, z, core) for dy in range(2)]
    for peer in peers:
        pl.semaphore_signal(barrier, inc=1, device_id=peer, device_id_type=MESH)
    for copy in exps:
        copy.wait()
    for k in range(3):
        line = jnp.exp2(wexp[pl.ds(128 * k, 128)].astype(F32)).reshape(1, 128)
        w_ref[pl.ds(128 * k, 128)] = jnp.broadcast_to(line, (128, 128)).T.astype(jnp.bfloat16)

    def remote(src, dst, send, recv, to):
        return pltpu.make_async_remote_copy(src_ref=src, dst_ref=dst, send_sem=send, recv_sem=recv,
                                            device_id=to, device_id_type=MESH)

    def halves(s, part):
        at = pl.ds(s * 8 + part * 4, 4)
        return remote(g.at[1 - core, :, at], pr.at[:, at], dsend, drecv.at[s, part], partner)

    def mine(col, first, count):
        return g.at[core, col, pl.ds(first, count)]

    def to_right(col, src, dst, sem):
        remote(src, dst, ssem.at[col, 0], sem, right[col]).start()

    def to_left(col, src, dst, sem):
        remote(src, dst, ssem.at[col, 1], sem, left[col]).start()

    def final_right(col, stage, first, count, at):
        to_right(col, mine(col, first, count), fl.at[col, pl.ds(at, count)], fsem.at[col, 0, stage])

    def final_left(col, stage, first, count, at):
        to_left(col, mine(col, first, count), fr.at[col, pl.ds(at, count)], fsem.at[col, 1, stage])

    def relay_right(col, first, count, at, sem):
        to_right(col, mine(col, first, count), rl.at[col, pl.ds(at, count)], rsem.at[0, sem])

    def relay_left(col, first, count, at, sem):
        to_left(col, mine(col, first, count), rr.at[col, pl.ds(at, count)], rsem.at[1, sem])

    def taken(buf, side, col, first, count, at, sem):
        part = buf.at[col, pl.ds(at, count)]
        remote(part, part, ssem.at[col, 0], rsem.at[side, sem], right[col]).wait_recv()
        g[core, col, pl.ds(first, count)] += buf[col, pl.ds(at, count)]

    def grams(s):
        for i in range(8):
            fetch(s, i).wait()

        w = w_ref[...]
        w3 = jnp.concatenate([w, w, w], axis=1)
        for i in range(8):
            t = xb[s % 2, i]
            tw = t * w3
            low = tdot(t[:, :256], tw[:, :256])
            high = tdot(t[:, 256:], tw[:, 128:])

            def put(half, col, row, value):
                g[half, col, s * 8 + i, pl.ds(row, value.shape[0]), :] = value

            pack(low, high, put)
            if i == 3:
                @pl.when(s == 0)
                def _():
                    pl.semaphore_wait(barrier, len(peers))

                halves(s, 0).start()

        halves(s, 1).start()

    def summed(s):
        base = s * 8
        halves(s, 0).wait_recv()
        halves(s, 1).wait_recv()
        for col in range(3):
            g[core, col, pl.ds(base, 8)] += pr[col, pl.ds(base, 8)]
        xs, yh = order(s)

        @pl.when(xs == 0)
        def _():
            relay_right(0, base, 4, yh * 4, yh)
            relay_left(0, base + 4, 4, yh * 4, yh)

        @pl.when(xs == 1)
        def _():
            final_right(0, 0, base + 4, 4, yh * 8 + 4)

        @pl.when(xs == 2)
        def _():
            final_left(0, 0, base, 4, yh * 8)

        @pl.when(yh == 0)
        def _():
            relay_right(1, base, 2, xs * 2, 2 + xs)
            relay_left(1, base + 2, 2, xs * 2, 2 + xs)
            final_right(1, xs, base + 6, 2, xs * 4 + 2)

        @pl.when(yh == 1)
        def _():
            final_left(1, xs, base, 2, xs * 4)

        relay_right(2, base, 1, s, 6 + s)
        relay_left(2, base + 4, 1, s, 6 + s)
        final_right(2, yh * (1 + xs // 2), base + 5, 1, yh * 8 + 4 + xs)
        final_left(2, yh * (1 + xs // 2), base + 2, 1, yh * 8 + xs)

    def passed_x(s):
        base = s * 8
        xs, yh = order(s)

        @pl.when(xs == 1)
        def _():
            taken(rl, 0, 0, base, 4, yh * 4, yh)
            final_right(0, 0, base, 4, yh * 8)

        @pl.when(xs == 2)
        def _():
            taken(rr, 1, 0, base + 4, 4, yh * 4, yh)
            final_left(0, 0, base + 4, 4, yh * 8 + 4)

    def passed_yz(s):
        base = s * 8
        xs, yh = order(s)

        @pl.when(yh == 0)
        def _():
            taken(rl, 0, 1, base + 4, 2, xs * 2, 2 + xs)
            final_right(1, xs, base + 4, 2, xs * 4)

        @pl.when(yh == 1)
        def _():
            taken(rr, 1, 1, base + 2, 2, xs * 2, 2 + xs)
            final_left(1, xs, base + 2, 2, xs * 4 + 2)

        taken(rl, 0, 2, base + 1, 1, s, 6 + s)
        final_right(2, yh * (1 + xs // 2), base + 1, 1, yh * 8 + xs)
        taken(rr, 1, 2, base + 6, 1, s, 6 + s)
        final_left(2, yh * (1 + xs // 2), base + 6, 1, yh * 8 + 4 + xs)

    def step(s, carry):
        @pl.when(s < 7)
        def _():
            for i in range(8):
                fetch(s + 1, i).start()

        grams(s)

        @pl.when(s >= 1)
        def _():
            summed(s - 1)

        @pl.when(s >= LAG_X)
        def _():
            passed_x(s - LAG_X)

        @pl.when(s >= LAG)
        def _():
            passed_yz(s - LAG)

        return carry

    lax.fori_loop(0, 8, step, 0)
    summed(7)

    def rest(s, carry):
        pl.when(s >= 8 - LAG_X)(lambda: passed_x(s))
        passed_yz(s)
        return carry

    lax.fori_loop(8 - LAG, 8, rest, 0)

    axis2, axis3 = (2, 0, 1), (1, 2, 0)
    hops = (far, right, left)

    def arrived(col, stage, first, count):
        for buf, side, to in ((fl, 0, left), (fr, 1, right)):
            whole = buf.at[col, pl.ds(first, count)]
            remote(whole, whole, ssem.at[col, side], fsem.at[col, side, stage], to[col]).wait_recv()

    def complete(col, u, v):
        group, i, at = (
            ((3, v // 2), v % 2 * 4 + u, v * 4 + u),
            ((u, 1), 4 + v, u * 4 + v),
            ((v, u // 2), 3 + 4 * (u % 2), u * 4 + v),
        )[col]
        f1[col, u, v] = g[core, col, GROUPS.index(group) * 8 + i] + fl[col, at] + fr[col, at]

    def second(col, u, first, count):
        rows = pl.ds(first, count)
        remote(f1.at[col, u, rows], q2.at[col, u, rows], s2send, q2sem.at[col, u], hops[u][axis2[col]]).start()

    def along_x(u):
        arrived(1, u, u * 4, 4)
        for v in range(4):
            complete(1, u, v)
        if u < 3:
            second(1, u, 0, 4)

    arrived(0, 0, 0, 16)
    for u in range(4):
        for v in range(4):
            complete(0, u, v)
        if u < 3:
            second(0, u, 0, 4)
    along_x(0)
    arrived(2, 0, 0, 8)
    for u in range(2):
        for v in range(4):
            complete(2, u, v)
        second(2, u, 0, 4)
    along_x(1)
    for k in range(2):
        arrived(2, 1 + k, 8, 4)
        for v in range(2 * k, 2 * k + 2):
            for u in range(2, 4):
                complete(2, u, v)
        second(2, 2, 2 * k, 2)
        along_x(2 + k)
    for col in range(3):
        for u in range(3):
            remote(q2.at[col, u], q2.at[col, u], s2send, q2sem.at[col, u], right[col]).wait_recv()
        f2[col] = (f1[col, 3] + q2[col, 0]) + (q2[col, 1] + q2[col, 2])
        for k, to in enumerate(hops):
            remote(f2.at[col, k], f3.at[col, k], s3send.at[col, k], s3sem.at[col, k], to[axis3[col]]).start()
    for col in range(3):
        for k, to in enumerate((far, right, left)):
            remote(f2.at[col, k], f3.at[col, k], s3send.at[col, k], s3sem.at[col, k], to[axis3[col]]).wait_recv()
        h[core, col] = (f2[col, 3] + f3[col, 0]) + (f3[col, 1] + f3[col, 2])
    both = remote(h.at[core], h.at[core], hsem.at[0], hsem.at[1], partner)
    both.start()
    both.wait_recv()
    flat = jnp.concatenate([h[half, col] for half in range(2) for col in range(3)], axis=0)
    owner = (x * 16 + y * 4 + z) * 2 + core
    lane = lax.broadcasted_iota(jnp.int32, (1, 128), 1)
    exponent = jnp.where(lane == owner, dexp[...].astype(F32).reshape(1, 128), 0.0)
    scale = jnp.exp2(-jnp.sum(exponent, axis=1, keepdims=True))
    slot = z * 2 + core

    def emit(first, count, value):
        rows = pl.ds(first, count)
        own[rows] = value
        for k in range(8):
            to = device(x, base_y + (low_y + 1 - k // 4) % 2, (z + (2, 1, 3, 0)[k % 4]) % 4, low_y)
            copy = remote(own.at[rows], got.at[slot, rows], asem, bsem.at[slot], to)
            if k < 7:
                copy.start()
            else:
                pl.when(core != low_y)(copy.start)

        @pl.when(core == low_y)
        def _():
            got[slot, rows] = value

    whiten(flat, core == 0, scale, total, emit)

    for j in range(8):
        @pl.when(jnp.logical_or(core != low_y, slot != j))
        def _():
            remote(got.at[j], got.at[j], asem, bsem.at[j], partner).wait_recv()

    for col in range(3):
        for side in range(2):
            sent = g.at[core, col, pl.ds(0, 24)]
            remote(sent, sent, ssem.at[col, side], fsem.at[col, side, 0], right[col]).wait_send()
        for k in range(3):
            remote(f2.at[col, k], f3.at[col, k], s3send.at[col, k], s3sem.at[col, k], right[col]).wait_send()
    ahead = g.at[core, 0, pl.ds(0, 36)]
    remote(ahead, ahead, s2send, q2sem.at[0, 0], partner).wait_send()
    every = g.at[1 - core]
    remote(every, pr, dsend, drecv.at[0, 0], partner).wait_send()
    both.wait_send()
    seven = got.at[pl.ds(0, 7)]
    remote(seven, seven, asem, bsem.at[0], partner).wait_send()

    @pl.when(core != low_y)
    def _():
        remote(got.at[0], got.at[0], asem, bsem.at[0], partner).wait_send()


def unpack_kernel(packed, out_ref, full, sem):
    copies = []
    for j in range(8):
        full[j, 0:32, 0:64] = packed[j, 0:32, 0:64]
        full[j, 32:64, 0:64] = packed[j, 0:32, 64:128]
        full[j, 0:64, 64:192] = jnp.zeros((64, 128), F32)
        full[j, 64:128, 0:128] = packed[j, 32:96]
        full[j, 64:128, 128:192] = jnp.zeros((64, 64), F32)
        full[j, 128:192, 0:128] = packed[j, 96:160]
        full[j, 128:160, 128:192] = packed[j, 160:192, 0:64]
        full[j, 160:192, 128:192] = packed[j, 160:192, 64:128]
        copies.append(pltpu.make_async_copy(full.at[j], out_ref.at[j], sem.at[j]))
        copies[-1].start()
    for copy in copies:
        copy.wait()


def on_device(projected, weight_exp, damp_exp):
    total = projected.shape[0] * lax.axis_size('dp') * lax.axis_size('head')
    unit = (ROWS, 128)
    dma = pltpu.SemaphoreType.DMA
    packed = pl.pallas_call(
        functools.partial(whitening_kernel, total),
        out_shape=OUT((8, HD, 128), F32),
        in_specs=[pl.BlockSpec(memory_space=pl.ANY), pl.BlockSpec(memory_space=pl.ANY),
                  pl.BlockSpec(memory_space=pl.ANY)],
        out_specs=pl.BlockSpec(memory_space=pltpu.VMEM),
        scratch_shapes=[
            pltpu.VMEM((384,), jnp.int32), pltpu.VMEM((128,), jnp.int32), pltpu.VMEM((384, 128), jnp.bfloat16), dma((2,)),
            pltpu.VMEM((HD, 128), F32), dma, dma((8,)),
            pltpu.VMEM((2, 8, 384, 384), jnp.bfloat16),
            pltpu.VMEM((2, 3, 64) + unit, F32),
            pltpu.VMEM((3, 64) + unit, F32),
            pltpu.VMEM((3, 8) + unit, F32),
            pltpu.VMEM((3, 8) + unit, F32),
            pltpu.VMEM((3, 16) + unit, F32),
            pltpu.VMEM((3, 16) + unit, F32),
            pltpu.VMEM((3, 4, 4) + unit, F32),
            pltpu.VMEM((3, 3, 4) + unit, F32),
            pltpu.VMEM((3, 4) + unit, F32),
            pltpu.VMEM((3, 3) + unit, F32),
            pltpu.VMEM((2, 3) + unit, F32),
            dma((2, 8)), dma, dma((8, 2)), dma((2, 14)), dma((3, 2)), dma((3, 2, 4)),
            dma, dma((3, 3)), dma((3, 3)), dma((3, 3)), dma((2,)),
        ],
        compiler_params=pltpu.CompilerParams(collective_id=0, has_side_effects=True, vmem_limit_bytes=58 * 2**20),
        name="whitening",
    )(projected, weight_exp, damp_exp)
    return pl.pallas_call(
        unpack_kernel,
        out_shape=jax.ShapeDtypeStruct((8, HD, HD), F32),
        in_specs=[pl.BlockSpec(memory_space=pltpu.VMEM)],
        out_specs=pl.BlockSpec(memory_space=pl.ANY),
        scratch_shapes=[pltpu.VMEM((8, HD, HD), F32), dma((8,))],
        name="unpack",
    )(pltpu.with_memory_space_constraint(packed, pltpu.VMEM))


def solution(mesh):
    return jax.shard_map(
        on_device,
        mesh=mesh,
        in_specs=(P(("dp", "head"), None), P(("dp", "head")), P()),
        out_specs=P("head", None, None),
        check_vma=False,
    )
```

```python
import functools
import jax
import jax.numpy as jnp
from jax import lax
from jax.experimental import pallas as pl
from jax.experimental.pallas import tpu as pltpu
from jax.sharding import PartitionSpec as P

HD = 192
ROWS = 56
SIZE = (48, 56, 48)
START = (0, 48, 104)
HALF = 152
OUT = pltpu.VMEM
LAG = 4
MESH = pl.DeviceIdType.MESH
F32 = jnp.float32


def tdot(a, b):
    return lax.dot_general(a, b, (((0,), (0,)), ((), ())), preferred_element_type=F32)


def place():
    dp, head = lax.axis_index("dp"), lax.axis_index("head")
    x, y, z = head // 4, (head // 2) % 2 * 2 + dp // 4, dp % 4
    return x, y, z, head % 2


def device(x, y, z, core):
    return (y % 2 * 4 + z, x * 4 + y // 2 * 2 + core)


GROUPS = ((0, 0), (0, 1), (1, 0), (2, 0), (1, 1), (3, 0), (2, 1), (3, 1))


def order(s):
    xs = sum(x << (2 * i) for i, (x, _) in enumerate(GROUPS))
    ys = sum(y << i for i, (_, y) in enumerate(GROUPS))
    return lax.shift_right_logical(jnp.int32(xs), jnp.int32(2 * s)) % 4, lax.shift_right_logical(jnp.int32(ys), jnp.int32(s)) % 2


def rel(step):
    return (2 - step + (step // 2) * (7 - 2 * step)) % 4


def pack(low, high, put):
    r = lax.broadcasted_iota(jnp.int32, (128, 128), 0)
    c = lax.broadcasted_iota(jnp.int32, (128, 128), 1)
    odd = high[:, 128:]
    left = c < 64
    a = jnp.where(r >= c, low[:128, :128], odd)
    b = jnp.where(left, low[:128, 128:], high[:, :128])
    top, turned = low[128:160, 128:], low[160:192, 128:]
    upper, under = low[192:224, 128:], low[224:, 128:]
    r32, c32 = r[:32], c[:32] % 64
    e = jnp.where(left[:32], jnp.where(r32 >= c32, top, pltpu.roll(upper, 64, 1)),
                  jnp.where(r32 + 32 >= c32, pltpu.roll(turned, 64, 1), under))
    d = jnp.sum(jnp.where(r == c, odd, 0.0), axis=0, keepdims=True)
    d2 = jnp.sum(jnp.where(r32 == c32, upper, 0.0) + jnp.where(r32 + 32 == c32, under, 0.0), axis=0, keepdims=True)
    first = 0
    for value in (a, b, e, jnp.where(r[:16] == 0, d, d2)):
        while value.shape[0]:
            half, at = divmod(first, HALF)
            col = sum(at >= start for start in START) - 1
            count = min(value.shape[0], START[col] + SIZE[col] - at)
            put(half, col, at - START[col], value[:count])
            value, first = value[count:], first + count


def dot(a, b, ca, cb):
    return lax.dot_general(a, b, (((ca,), (cb,)), ((), ())), precision=lax.Precision.HIGHEST,
                           preferred_element_type=F32)


def mul(a, b):
    return dot(a, b, 1, 0)


def mul_t(a, b):
    return dot(a, b, 1, 1)


def inverse_factor(d, width=16):
    r = lax.broadcasted_iota(jnp.int32, (64, 64), 0)
    c = lax.broadcasted_iota(jnp.int32, (64, 64), 1)
    full = jnp.concatenate([d, (r == c).astype(F32)], axis=1)
    m = [full[8 * i:8 * i + 8] for i in range(8)]
    sub = lax.broadcasted_iota(jnp.int32, (8, 128), 0)
    diag = [jnp.ones((8, 128), F32) for _ in range(8)]

    def row(v, j):
        return jnp.broadcast_to(v[j:j + 1], (8, 128))

    for base in range(0, 64, width):
        cs = {(i, n): jnp.broadcast_to(m[i][:, n:n + 1], (8, 128))
              for i in range(base // 8, 8) for n in range(base, base + width)}
        for j in range(base, base + width, 2):
            q, p = j // 8, j % 8
            a, b, e = row(cs[q, j], p), row(cs[q, j + 1], p), row(cs[q, j + 1], p + 1)
            det = a * e - b * b
            inv, over = 1.0 / det, 1.0 / a
            ei, bi, ai = e * inv, b * inv, a * inv
            r0, r1 = row(m[q], p), row(m[q], p + 1)
            t0, t1 = ei * r0 - bi * r1, ai * r1 - bi * r0
            second = jnp.where(sub == p + 1, b * over * r0, 0.0)
            diag[q] = jnp.where(sub == p, a, jnp.where(sub == p + 1, det * over, diag[q]))
            us = {}
            for n in range(j + 2, base + width):
                c0, c1 = row(cs[q, n], p), row(cs[q, n], p + 1)
                us[n] = (ei * c0 - bi * c1, ai * c1 - bi * c0)
            for i in range(q, 8):
                f0, f1 = cs[i, j], cs[i, j + 1]
                if i == q:
                    f0, f1 = jnp.where(sub > p + 1, f0, 0.0), jnp.where(sub > p + 1, f1, 0.0)
                    m[i] = m[i] - (f0 * t0 + f1 * t1 + second)
                else:
                    m[i] = m[i] - (f0 * t0 + f1 * t1)
                for n in range(j + 2, base + width):
                    cs[i, n] = cs[i, n] - (f0 * us[n][0] + f1 * us[n][1])
    return jnp.concatenate([(m[i] * lax.rsqrt(diag[i]))[:, 64:] for i in range(8)], axis=0)


def folded(a):
    return jnp.concatenate([a[:32], a[32:]], axis=1)


def whiten(flat, even, scale, total, emit):
    r = lax.broadcasted_iota(jnp.int32, (128, 128), 0)
    c = lax.broadcasted_iota(jnp.int32, (128, 128), 1)
    flat = flat / total
    a, b, e, lines = flat[:128], flat[128:256], flat[256:288], flat[288:296]
    t = a.T
    low = jnp.where(r >= c, a, t)
    high = jnp.where(r < c, a, jnp.where(r == c, lines[0:1], t))
    a = jnp.where(even, low, high)
    b = jnp.where(even, b[:, :64], b[:, 64:])
    b0, b1 = b[:64], b[64:]
    e = jnp.concatenate([e[:, :64], e[:, 64:]], axis=0)
    rs, cc = r[:64, :64], c[:64, :64]
    corner = jnp.where(even, jnp.where(rs >= cc, e, e.T),
                       jnp.where(rs < cc, e, jnp.where(rs == cc, lines[1:2, 64:], e.T)))
    a00, a10, a11 = a[:64, :64], a[64:, :64], a[64:, 64:]
    g00 = jnp.where(even, a00, corner)
    g10 = jnp.where(even, a10, b0)
    g11 = jnp.where(even, a11, a00)
    g20 = jnp.where(even, b0.T, b1)
    g21 = jnp.where(even, b1.T, a10)
    g22 = jnp.where(even, corner, a11)
    eye = r[:64, :64] == c[:64, :64]
    diag = jnp.where(eye, g00 + g11 + g22, 0.0)
    level = jnp.sum(jnp.sum(diag, axis=0, keepdims=True), axis=1, keepdims=True) / HD + 1e-06
    damp = jnp.where(eye, scale * level, 0.0)

    w00 = inverse_factor(g00 + damp)
    emit(0, 32, folded(w00))
    l10, l20 = mul_t(g10, w00), mul_t(g20, w00)
    s11 = g11 + damp - mul_t(l10, l10)
    s21 = g21 - mul_t(l20, l10)
    s22 = g22 + damp - mul_t(l20, l20)
    x10, x20 = mul(l10, w00), mul(l20, w00)
    w11 = inverse_factor(s11)
    l21 = mul_t(s21, w11)
    s22 = s22 - mul_t(l21, l21)
    w10 = -mul(w11, x10)
    emit(32, 64, jnp.concatenate([w10, w11], axis=1))
    x21 = mul(l21, w11)
    x20 = x20 + mul(l21, w10)
    w22 = inverse_factor(s22)
    last = jnp.concatenate([-mul(w22, x20), -mul(w22, x21)], axis=1)
    emit(96, 96, jnp.concatenate([last, folded(w22)], axis=0))


def whitening_kernel(total, x_ref, weight_ref, damp_ref, got, wexp, dexp, w_ref, esem, own, asem, bsem, xb, g, pr, rl, rr, fl, fr, f1, q2, f2, f3, h,
                  xsem, dsend, drecv, rsem, ssem, fsem, s2send, q2sem, s3send, s3sem, hsem):
    x, y, z, core = place()
    partner = device(x, y, z, 1 - core)
    right = (device((x + 1) % 4, y, z, core), device(x, (y + 1) % 4, z, core), device(x, y, (z + 1) % 4, core))
    left = (device((x + 3) % 4, y, z, core), device(x, (y + 3) % 4, z, core), device(x, y, (z + 3) % 4, core))
    far = (device((x + 2) % 4, y, z, core), device(x, (y + 2) % 4, z, core), device(x, y, (z + 2) % 4, core))

    def fetch(s, i):
        xs, yh = order(s)
        px = (x + rel(xs)) % 4
        py = (y + rel(yh * 2 + i // 4)) % 4
        pz = (z + rel(i % 4)) % 4
        col = pl.multiple_of((px * 16 + py * 4 + pz) * 384, 384)
        return pltpu.make_async_copy(x_ref.at[:, pl.ds(col, 384)], xb.at[s % 2, i], xsem.at[s % 2, i])

    for i in range(8):
        fetch(0, i).start()

    exps = (pltpu.make_async_copy(weight_ref, wexp, esem.at[0]), pltpu.make_async_copy(damp_ref, dexp, esem.at[1]))
    for copy in exps:
        copy.start()

    barrier = pltpu.get_barrier_semaphore()
    base_y, low_y = y // 2 * 2, y % 2
    peers = [device(x, base_y + dy, (z + dz) % 4, cc) for dy in range(2) for dz in range(1, 4) for cc in range(2)]
    peers += [partner, device(x, base_y + 1 - low_y, z, 0), device(x, base_y + 1 - low_y, z, 1)]
    peers += [device((x + k) % 4, y, z, core) for k in range(1, 4)]
    peers += [device(x, (base_y + 2) % 4 + dy, z, core) for dy in range(2)]
    for peer in peers:
        pl.semaphore_signal(barrier, inc=1, device_id=peer, device_id_type=MESH)
    for copy in exps:
        copy.wait()
    for k in range(3):
        line = jnp.exp2(wexp[pl.ds(128 * k, 128)].astype(F32)).reshape(1, 128)
        w_ref[pl.ds(128 * k, 128)] = jnp.broadcast_to(line, (128, 128)).T.astype(jnp.bfloat16)

    def remote(src, dst, send, recv, to):
        return pltpu.make_async_remote_copy(src_ref=src, dst_ref=dst, send_sem=send, recv_sem=recv,
                                            device_id=to, device_id_type=MESH)

    def halves(s, part):
        at = pl.ds(s * 8 + part * 4, 4)
        return [remote(g.at[1 - core, col, at, pl.ds(0, SIZE[col])], pr.at[col, at, pl.ds(0, SIZE[col])], dsend.at[col],
                       drecv.at[s, part, col], partner) for col in range(3)]

    def mine(col, first, count):
        return g.at[core, col, pl.ds(first, count), pl.ds(0, SIZE[col])]

    def to_right(col, src, dst, sem):
        remote(src, dst, ssem.at[col, 0], sem, right[col]).start()

    def to_left(col, src, dst, sem):
        remote(src, dst, ssem.at[col, 1], sem, left[col]).start()

    def final_right(col, stage, first, count, at):
        to_right(col, mine(col, first, count), fl.at[col, pl.ds(at, count), pl.ds(0, SIZE[col])], fsem.at[col, 0, stage])

    def final_left(col, stage, first, count, at):
        to_left(col, mine(col, first, count), fr.at[col, pl.ds(at, count), pl.ds(0, SIZE[col])], fsem.at[col, 1, stage])

    def relay_right(col, first, count, at, sem):
        to_right(col, mine(col, first, count), rl.at[col, pl.ds(at, count), pl.ds(0, SIZE[col])], rsem.at[0, sem])

    def relay_left(col, first, count, at, sem):
        to_left(col, mine(col, first, count), rr.at[col, pl.ds(at, count), pl.ds(0, SIZE[col])], rsem.at[1, sem])

    def taken(buf, side, col, first, count, at, sem):
        rows = pl.ds(0, SIZE[col])
        part = buf.at[col, pl.ds(at, count), rows]
        remote(part, part, ssem.at[col, 0], rsem.at[side, sem], right[col]).wait_recv()
        g[core, col, pl.ds(first, count), rows] += buf[col, pl.ds(at, count), rows]

    def grams(s):
        for i in range(4):
            fetch(s, i).wait()

        w = w_ref[...]
        w3 = jnp.concatenate([w, w, w], axis=1)
        for i in range(8):
            t = xb[s % 2, i]
            tw = t * w3
            low = tdot(t[:, :256], tw[:, :256])
            high = tdot(t[:, 256:], tw[:, 128:])

            def put(half, col, row, value):
                g[half, col, s * 8 + i, pl.ds(row, value.shape[0]), :] = value

            pack(low, high, put)
            if i == 3:
                @pl.when(s == 0)
                def _():
                    pl.semaphore_wait(barrier, len(peers))

                for copy in halves(s, 0):
                    copy.start()
                for n in range(4, 8):
                    fetch(s, n).wait()

        for copy in halves(s, 1):
            copy.start()

    def summed(s):
        base = s * 8
        for copy in halves(s, 0) + halves(s, 1):
            copy.wait_recv()
        for col in range(3):
            g[core, col, pl.ds(base, 8), pl.ds(0, SIZE[col])] += pr[col, pl.ds(base, 8), pl.ds(0, SIZE[col])]
        xs, yh = order(s)

        @pl.when(xs == 0)
        def _():
            relay_right(0, base, 4, yh * 4, yh)
            relay_left(0, base + 4, 4, yh * 4, yh)

        @pl.when(xs == 1)
        def _():
            final_right(0, yh, base + 4, 4, yh * 8 + 4)

        @pl.when(xs == 2)
        def _():
            final_left(0, yh, base, 4, yh * 8)

        @pl.when(yh == 0)
        def _():
            relay_right(1, base, 2, xs * 2, 2 + xs)
            relay_left(1, base + 2, 2, xs * 2, 2 + xs)
            final_right(1, xs, base + 6, 2, xs * 4 + 2)

        @pl.when(yh == 1)
        def _():
            final_left(1, xs, base, 2, xs * 4)

        relay_right(2, base, 1, s, 6 + s)
        relay_left(2, base + 4, 1, s, 6 + s)
        final_right(2, yh * (1 + xs // 2), base + 5, 1, yh * 8 + 4 + xs)
        final_left(2, yh * (1 + xs // 2), base + 2, 1, yh * 8 + xs)

    def passed_x(s):
        base = s * 8
        xs, yh = order(s)

        @pl.when(xs == 1)
        def _():
            taken(rl, 0, 0, base, 4, yh * 4, yh)
            final_right(0, yh, base, 4, yh * 8)

        @pl.when(xs == 2)
        def _():
            taken(rr, 1, 0, base + 4, 4, yh * 4, yh)
            final_left(0, yh, base + 4, 4, yh * 8 + 4)

    def passed_yz(s):
        base = s * 8
        xs, yh = order(s)

        @pl.when(yh == 0)
        def _():
            taken(rl, 0, 1, base + 4, 2, xs * 2, 2 + xs)
            final_right(1, xs, base + 4, 2, xs * 4)

        @pl.when(yh == 1)
        def _():
            taken(rr, 1, 1, base + 2, 2, xs * 2, 2 + xs)
            final_left(1, xs, base + 2, 2, xs * 4 + 2)

        taken(rl, 0, 2, base + 1, 1, s, 6 + s)
        final_right(2, yh * (1 + xs // 2), base + 1, 1, yh * 8 + xs)
        taken(rr, 1, 2, base + 6, 1, s, 6 + s)
        final_left(2, yh * (1 + xs // 2), base + 6, 1, yh * 8 + 4 + xs)

    def step(s, carry):
        @pl.when(s < 7)
        def _():
            for i in range(8):
                fetch(s + 1, i).start()

        grams(s)

        @pl.when(s >= 1)
        def _():
            summed(s - 1)

        @pl.when(s == 5)
        def _():
            passed_x(2)

        @pl.when(s == 5)
        def _():
            passed_x(3)

        @pl.when(s == 7)
        def _():
            passed_x(4)
            passed_x(6)

        @pl.when(s >= LAG)
        def _():
            passed_yz(s - LAG)

        return carry

    lax.fori_loop(0, 8, step, 0)
    summed(7)

    def rest(s, carry):
        passed_yz(s)
        return carry

    lax.fori_loop(8 - LAG, 8, rest, 0)

    axis2, axis3 = (2, 0, 1), (1, 2, 0)
    hops = (far, right, left)

    def arrived(col, stage, first, count):
        for buf, side, to in ((fl, 0, left), (fr, 1, right)):
            whole = buf.at[col, pl.ds(first, count), pl.ds(0, SIZE[col])]
            remote(whole, whole, ssem.at[col, side], fsem.at[col, side, stage], to[col]).wait_recv()

    def complete(col, u, v):
        group, i, at = (
            ((3, v // 2), v % 2 * 4 + u, v * 4 + u),
            ((u, 1), 4 + v, u * 4 + v),
            ((v, u // 2), 3 + 4 * (u % 2), u * 4 + v),
        )[col]
        rows = pl.ds(0, SIZE[col])
        f1[col, u, v, rows] = g[core, col, GROUPS.index(group) * 8 + i, rows] + fl[col, at, rows] + fr[col, at, rows]

    def second(col, u, first, count):
        part = (pl.ds(first, count), pl.ds(0, SIZE[col]))
        remote(f1.at[(col, u) + part], q2.at[(col, u) + part], s2send.at[col], q2sem.at[col, u], hops[u][axis2[col]]).start()

    def along_x(u):
        arrived(1, u, u * 4, 4)
        for v in range(4):
            complete(1, u, v)
        if u < 3:
            second(1, u, 0, 4)

    def along_z(half):
        arrived(0, half, half * 8, 8)
        for u in range(4):
            for v in range(2 * half, 2 * half + 2):
                complete(0, u, v)
            if u < 3:
                second(0, u, 2 * half, 2)

    along_z(0)
    along_x(0)
    arrived(2, 0, 0, 8)
    for u in range(2):
        for v in range(4):
            complete(2, u, v)
        second(2, u, 0, 4)
    along_x(1)
    along_z(1)
    for k in range(2):
        arrived(2, 1 + k, 8, 4)
        for v in range(2 * k, 2 * k + 2):
            for u in range(2, 4):
                complete(2, u, v)
        second(2, 2, 2 * k, 2)
        along_x(2 + k)
    def third(col, k):
        rows = pl.ds(0, SIZE[col])
        return remote(f2.at[col, k, rows], f3.at[col, k, rows], s3send.at[col, k], s3sem.at[col, k], hops[k][axis3[col]])

    for col in range(3):
        rows = pl.ds(0, SIZE[col])
        for u in range(3):
            part = q2.at[col, u, :, rows]
            remote(part, part, s2send.at[col], q2sem.at[col, u], right[col]).wait_recv()
        f2[col, :, rows] = (f1[col, 3, :, rows] + q2[col, 0, :, rows]) + (q2[col, 1, :, rows] + q2[col, 2, :, rows])
        for k in range(3):
            third(col, k).start()
    for col in range(3):
        rows = pl.ds(0, SIZE[col])
        for k in range(3):
            third(col, k).wait_recv()
        h[core, pl.ds(START[col], SIZE[col])] = (f2[col, 3, rows] + f3[col, 0, rows]) + (f3[col, 1, rows] + f3[col, 2, rows])
    both = remote(h.at[core], h.at[core], hsem.at[0], hsem.at[1], partner)
    both.start()
    both.wait_recv()
    flat = jnp.concatenate([h[0], h[1]], axis=0)
    owner = (x * 16 + y * 4 + z) * 2 + core
    lane = lax.broadcasted_iota(jnp.int32, (1, 128), 1)
    exponent = jnp.where(lane == owner, dexp[...].astype(F32).reshape(1, 128), 0.0)
    scale = jnp.exp2(-jnp.sum(exponent, axis=1, keepdims=True))
    slot = z * 2 + core

    def emit(first, count, value):
        rows = pl.ds(first, count)
        own[rows] = value
        for k in range(8):
            to = device(x, base_y + (low_y + 1 - k // 4) % 2, (z + (2, 1, 3, 0)[k % 4]) % 4, low_y)
            copy = remote(own.at[rows], got.at[slot, rows], asem, bsem.at[slot], to)
            if k < 7:
                copy.start()
            else:
                pl.when(core != low_y)(copy.start)

        @pl.when(core == low_y)
        def _():
            got[slot, rows] = value

    whiten(flat, core == 0, scale, total, emit)

    for j in range(8):
        @pl.when(jnp.logical_or(core != low_y, slot != j))
        def _():
            remote(got.at[j], got.at[j], asem, bsem.at[j], partner).wait_recv()

    for col in range(3):
        for side in range(2):
            sent = g.at[core, col, pl.ds(0, 24), pl.ds(0, SIZE[col])]
            remote(sent, sent, ssem.at[col, side], fsem.at[col, side, 0], right[col]).wait_send()
        ahead = g.at[core, col, pl.ds(0, 12), pl.ds(0, SIZE[col])]
        remote(ahead, ahead, s2send.at[col], q2sem.at[col, 0], right[col]).wait_send()
        for k in range(3):
            third(col, k).wait_send()
    for col in range(3):
        every = g.at[1 - core, col, :, pl.ds(0, SIZE[col])]
        remote(every, every, dsend.at[col], drecv.at[0, 0, col], partner).wait_send()
    both.wait_send()
    seven = got.at[pl.ds(0, 7)]
    remote(seven, seven, asem, bsem.at[0], partner).wait_send()

    @pl.when(core != low_y)
    def _():
        remote(got.at[0], got.at[0], asem, bsem.at[0], partner).wait_send()


def unpack_kernel(packed, out_ref, full, sem):
    copies = []
    for j in range(8):
        full[j, 0:32, 0:64] = packed[j, 0:32, 0:64]
        full[j, 32:64, 0:64] = packed[j, 0:32, 64:128]
        full[j, 0:64, 64:192] = jnp.zeros((64, 128), F32)
        full[j, 64:128, 0:128] = packed[j, 32:96]
        full[j, 64:128, 128:192] = jnp.zeros((64, 64), F32)
        full[j, 128:192, 0:128] = packed[j, 96:160]
        full[j, 128:160, 128:192] = packed[j, 160:192, 0:64]
        full[j, 160:192, 128:192] = packed[j, 160:192, 64:128]
        copies.append(pltpu.make_async_copy(full.at[j], out_ref.at[j], sem.at[j]))
        copies[-1].start()
    for copy in copies:
        copy.wait()


def on_device(projected, weight_exp, damp_exp):
    total = projected.shape[0] * lax.axis_size('dp') * lax.axis_size('head')
    unit = (ROWS, 128)
    dma = pltpu.SemaphoreType.DMA
    packed = pl.pallas_call(
        functools.partial(whitening_kernel, total),
        out_shape=OUT((8, HD, 128), F32),
        in_specs=[pl.BlockSpec(memory_space=pl.ANY), pl.BlockSpec(memory_space=pl.ANY),
                  pl.BlockSpec(memory_space=pl.ANY)],
        out_specs=pl.BlockSpec(memory_space=pltpu.VMEM),
        scratch_shapes=[
            pltpu.VMEM((384,), jnp.int32), pltpu.VMEM((128,), jnp.int32), pltpu.VMEM((384, 128), jnp.bfloat16), dma((2,)),
            pltpu.VMEM((HD, 128), F32), dma, dma((8,)),
            pltpu.VMEM((2, 8, 384, 384), jnp.bfloat16),
            pltpu.VMEM((2, 3, 64) + unit, F32),
            pltpu.VMEM((3, 64) + unit, F32),
            pltpu.VMEM((3, 8) + unit, F32),
            pltpu.VMEM((3, 8) + unit, F32),
            pltpu.VMEM((3, 16) + unit, F32),
            pltpu.VMEM((3, 16) + unit, F32),
            pltpu.VMEM((3, 4, 4) + unit, F32),
            pltpu.VMEM((3, 3, 4) + unit, F32),
            pltpu.VMEM((3, 4) + unit, F32),
            pltpu.VMEM((3, 3) + unit, F32),
            pltpu.VMEM((2, 152, 128), F32),
            dma((2, 8)), dma((3,)), dma((8, 2, 3)), dma((2, 14)), dma((3, 2)), dma((3, 2, 4)),
            dma((3,)), dma((3, 3)), dma((3, 3)), dma((3, 3)), dma((2,)),
        ],
        compiler_params=pltpu.CompilerParams(collective_id=0, has_side_effects=True, vmem_limit_bytes=58 * 2**20),
        name="whitening",
    )(projected, weight_exp, damp_exp)
    return pl.pallas_call(
        unpack_kernel,
        out_shape=jax.ShapeDtypeStruct((8, HD, HD), F32),
        in_specs=[pl.BlockSpec(memory_space=pltpu.VMEM)],
        out_specs=pl.BlockSpec(memory_space=pl.ANY),
        scratch_shapes=[pltpu.VMEM((8, HD, HD), F32), dma((8,))],
        name="unpack",
    )(pltpu.with_memory_space_constraint(packed, pltpu.VMEM))


def solution(mesh):
    return jax.shard_map(
        on_device,
        mesh=mesh,
        in_specs=(P(("dp", "head"), None), P(("dp", "head")), P()),
        out_specs=P("head", None, None),
        check_vma=False,
    )
```

```python
import functools
import jax
import jax.numpy as jnp
from jax import lax
from jax.experimental import pallas as pl
from jax.experimental.pallas import tpu as pltpu
from jax.sharding import PartitionSpec as P

HD = 192
ROWS = 56
SIZE = (48, 56, 48)
START = (0, 48, 104)
HALF = 152
OUT = pltpu.VMEM
LAG = 4
MESH = pl.DeviceIdType.MESH
F32 = jnp.float32


def tdot(a, b):
    return lax.dot_general(a, b, (((0,), (0,)), ((), ())), preferred_element_type=F32)


def place():
    dp, head = lax.axis_index("dp"), lax.axis_index("head")
    x, y, z = head // 4, (head // 2) % 2 * 2 + dp // 4, dp % 4
    return x, y, z, head % 2


def device(x, y, z, core):
    return (y % 2 * 4 + z, x * 4 + y // 2 * 2 + core)


GROUPS = ((0, 0), (0, 1), (1, 0), (2, 0), (1, 1), (3, 0), (2, 1), (3, 1))


def order(s):
    xs = sum(x << (2 * i) for i, (x, _) in enumerate(GROUPS))
    ys = sum(y << i for i, (_, y) in enumerate(GROUPS))
    return lax.shift_right_logical(jnp.int32(xs), jnp.int32(2 * s)) % 4, lax.shift_right_logical(jnp.int32(ys), jnp.int32(s)) % 2


def rel(step):
    return (2 - step + (step // 2) * (7 - 2 * step)) % 4


def pack(low, high, put):
    r = lax.broadcasted_iota(jnp.int32, (128, 128), 0)
    c = lax.broadcasted_iota(jnp.int32, (128, 128), 1)
    odd = high[:, 128:]
    left = c < 64
    a = jnp.where(r >= c, low[:128, :128], odd)
    b = jnp.where(left, low[:128, 128:], high[:, :128])
    top, turned = low[128:160, 128:], low[160:192, 128:]
    upper, under = low[192:224, 128:], low[224:, 128:]
    r32, c32 = r[:32], c[:32] % 64
    e = jnp.where(left[:32], jnp.where(r32 >= c32, top, pltpu.roll(upper, 64, 1)),
                  jnp.where(r32 + 32 >= c32, pltpu.roll(turned, 64, 1), under))
    d = jnp.sum(jnp.where(r == c, odd, 0.0), axis=0, keepdims=True)
    d2 = jnp.sum(jnp.where(r32 == c32, upper, 0.0) + jnp.where(r32 + 32 == c32, under, 0.0), axis=0, keepdims=True)
    first = 0
    for value in (a, b, e, jnp.where(r[:16] == 0, d, d2)):
        while value.shape[0]:
            half, at = divmod(first, HALF)
            col = sum(at >= start for start in START) - 1
            count = min(value.shape[0], START[col] + SIZE[col] - at)
            put(half, col, at - START[col], value[:count])
            value, first = value[count:], first + count


def dot(a, b, ca, cb):
    return lax.dot_general(a, b, (((ca,), (cb,)), ((), ())), precision=lax.Precision.HIGHEST,
                           preferred_element_type=F32)


def mul(a, b):
    return dot(a, b, 1, 0)


def mul_t(a, b):
    return dot(a, b, 1, 1)


def inverse_factor(d, width=16):
    r = lax.broadcasted_iota(jnp.int32, (64, 64), 0)
    c = lax.broadcasted_iota(jnp.int32, (64, 64), 1)
    full = jnp.concatenate([d, (r == c).astype(F32)], axis=1)
    m = [full[8 * i:8 * i + 8] for i in range(8)]
    sub = lax.broadcasted_iota(jnp.int32, (8, 128), 0)
    diag = [jnp.ones((8, 128), F32) for _ in range(8)]

    def row(v, j):
        return jnp.broadcast_to(v[j:j + 1], (8, 128))

    for base in range(0, 64, width):
        cs = {(i, n): jnp.broadcast_to(m[i][:, n:n + 1], (8, 128))
              for i in range(base // 8, 8) for n in range(base, base + width)}
        for j in range(base, base + width, 2):
            q, p = j // 8, j % 8
            a, b, e = row(cs[q, j], p), row(cs[q, j + 1], p), row(cs[q, j + 1], p + 1)
            det = a * e - b * b
            inv, over = 1.0 / det, 1.0 / a
            ei, bi, ai = e * inv, b * inv, a * inv
            r0, r1 = row(m[q], p), row(m[q], p + 1)
            t0, t1 = ei * r0 - bi * r1, ai * r1 - bi * r0
            second = jnp.where(sub == p + 1, b * over * r0, 0.0)
            diag[q] = jnp.where(sub == p, a, jnp.where(sub == p + 1, det * over, diag[q]))
            us = {}
            for n in range(j + 2, base + width):
                c0, c1 = row(cs[q, n], p), row(cs[q, n], p + 1)
                us[n] = (ei * c0 - bi * c1, ai * c1 - bi * c0)
            for i in range(q, 8):
                f0, f1 = cs[i, j], cs[i, j + 1]
                if i == q:
                    f0, f1 = jnp.where(sub > p + 1, f0, 0.0), jnp.where(sub > p + 1, f1, 0.0)
                    m[i] = m[i] - (f0 * t0 + f1 * t1 + second)
                else:
                    m[i] = m[i] - (f0 * t0 + f1 * t1)
                for n in range(j + 2, base + width):
                    cs[i, n] = cs[i, n] - (f0 * us[n][0] + f1 * us[n][1])
    return jnp.concatenate([(m[i] * lax.rsqrt(diag[i]))[:, 64:] for i in range(8)], axis=0)


def folded(a):
    return jnp.concatenate([a[:32], a[32:]], axis=1)


def whiten(flat, even, scale, total, emit):
    r = lax.broadcasted_iota(jnp.int32, (128, 128), 0)
    c = lax.broadcasted_iota(jnp.int32, (128, 128), 1)
    flat = flat / total
    a, b, e, lines = flat[:128], flat[128:256], flat[256:288], flat[288:296]
    t = a.T
    low = jnp.where(r >= c, a, t)
    high = jnp.where(r < c, a, jnp.where(r == c, lines[0:1], t))
    a = jnp.where(even, low, high)
    b = jnp.where(even, b[:, :64], b[:, 64:])
    b0, b1 = b[:64], b[64:]
    e = jnp.concatenate([e[:, :64], e[:, 64:]], axis=0)
    rs, cc = r[:64, :64], c[:64, :64]
    corner = jnp.where(even, jnp.where(rs >= cc, e, e.T),
                       jnp.where(rs < cc, e, jnp.where(rs == cc, lines[1:2, 64:], e.T)))
    a00, a10, a11 = a[:64, :64], a[64:, :64], a[64:, 64:]
    g00 = jnp.where(even, a00, corner)
    g10 = jnp.where(even, a10, b0)
    g11 = jnp.where(even, a11, a00)
    g20 = jnp.where(even, b0.T, b1)
    g21 = jnp.where(even, b1.T, a10)
    g22 = jnp.where(even, corner, a11)
    eye = r[:64, :64] == c[:64, :64]
    diag = jnp.where(eye, g00 + g11 + g22, 0.0)
    level = jnp.sum(jnp.sum(diag, axis=0, keepdims=True), axis=1, keepdims=True) / HD + 1e-06
    damp = jnp.where(eye, scale * level, 0.0)

    w00 = inverse_factor(g00 + damp)
    emit(0, 32, folded(w00))
    l10, l20 = mul_t(g10, w00), mul_t(g20, w00)
    s11 = g11 + damp - mul_t(l10, l10)
    s21 = g21 - mul_t(l20, l10)
    s22 = g22 + damp - mul_t(l20, l20)
    x10, x20 = mul(l10, w00), mul(l20, w00)
    w11 = inverse_factor(s11)
    l21 = mul_t(s21, w11)
    s22 = s22 - mul_t(l21, l21)
    w10 = -mul(w11, x10)
    emit(32, 64, jnp.concatenate([w10, w11], axis=1))
    x21 = mul(l21, w11)
    x20 = x20 + mul(l21, w10)
    w22 = inverse_factor(s22)
    emit(160, 32, folded(w22))
    emit(96, 64, jnp.concatenate([-mul(w22, x20), -mul(w22, x21)], axis=1))


def whitening_kernel(total, x_ref, weight_ref, damp_ref, got, wexp, dexp, w_ref, esem, own, asem, bsem, xb, g, pr, rl, rr, fl, fr, f1, q2, f2, f3, h,
                  xsem, dsend, drecv, rsem, ssem, fsem, s2send, q2sem, s3send, s3sem, hsem):
    x, y, z, core = place()
    partner = device(x, y, z, 1 - core)
    right = (device((x + 1) % 4, y, z, core), device(x, (y + 1) % 4, z, core), device(x, y, (z + 1) % 4, core))
    left = (device((x + 3) % 4, y, z, core), device(x, (y + 3) % 4, z, core), device(x, y, (z + 3) % 4, core))
    far = (device((x + 2) % 4, y, z, core), device(x, (y + 2) % 4, z, core), device(x, y, (z + 2) % 4, core))

    def fetch(s, i):
        xs, yh = order(s)
        px = (x + rel(xs)) % 4
        py = (y + rel(yh * 2 + i // 4)) % 4
        pz = (z + rel(i % 4)) % 4
        col = pl.multiple_of((px * 16 + py * 4 + pz) * 384, 384)
        return pltpu.make_async_copy(x_ref.at[:, pl.ds(col, 384)], xb.at[s % 2, i], xsem.at[s % 2, i])

    for i in range(8):
        fetch(0, i).start()

    exps = (pltpu.make_async_copy(weight_ref, wexp, esem.at[0]), pltpu.make_async_copy(damp_ref, dexp, esem.at[1]))
    for copy in exps:
        copy.start()

    barrier = pltpu.get_barrier_semaphore()
    base_y, low_y = y // 2 * 2, y % 2
    peers = [device(x, base_y + dy, (z + dz) % 4, cc) for dy in range(2) for dz in range(1, 4) for cc in range(2)]
    peers += [partner, device(x, base_y + 1 - low_y, z, 0), device(x, base_y + 1 - low_y, z, 1)]
    peers += [device((x + k) % 4, y, z, core) for k in range(1, 4)]
    peers += [device(x, (base_y + 2) % 4 + dy, z, core) for dy in range(2)]
    for peer in peers:
        pl.semaphore_signal(barrier, inc=1, device_id=peer, device_id_type=MESH)
    for copy in exps:
        copy.wait()
    for k in range(3):
        line = jnp.exp2(wexp[pl.ds(128 * k, 128)].astype(F32)).reshape(1, 128)
        w_ref[pl.ds(128 * k, 128)] = jnp.broadcast_to(line, (128, 128)).T.astype(jnp.bfloat16)

    def remote(src, dst, send, recv, to):
        return pltpu.make_async_remote_copy(src_ref=src, dst_ref=dst, send_sem=send, recv_sem=recv,
                                            device_id=to, device_id_type=MESH)

    def halves(s, part):
        at = pl.ds(s * 8 + part * 4, 4)
        return [remote(g.at[1 - core, col, at, pl.ds(0, SIZE[col])], pr.at[col, at, pl.ds(0, SIZE[col])], dsend.at[col],
                       drecv.at[s, part, col], partner) for col in range(3)]

    def mine(col, first, count):
        return g.at[core, col, pl.ds(first, count), pl.ds(0, SIZE[col])]

    def to_right(col, src, dst, sem):
        remote(src, dst, ssem.at[col, 0], sem, right[col]).start()

    def to_left(col, src, dst, sem):
        remote(src, dst, ssem.at[col, 1], sem, left[col]).start()

    def final_right(col, stage, first, count, at):
        to_right(col, mine(col, first, count), fl.at[col, pl.ds(at, count), pl.ds(0, SIZE[col])], fsem.at[col, 0, stage])

    def final_left(col, stage, first, count, at):
        to_left(col, mine(col, first, count), fr.at[col, pl.ds(at, count), pl.ds(0, SIZE[col])], fsem.at[col, 1, stage])

    def relay_right(col, first, count, at, sem):
        to_right(col, mine(col, first, count), rl.at[col, pl.ds(at, count), pl.ds(0, SIZE[col])], rsem.at[0, sem])

    def relay_left(col, first, count, at, sem):
        to_left(col, mine(col, first, count), rr.at[col, pl.ds(at, count), pl.ds(0, SIZE[col])], rsem.at[1, sem])

    def taken(buf, side, col, first, count, at, sem):
        rows = pl.ds(0, SIZE[col])
        part = buf.at[col, pl.ds(at, count), rows]
        remote(part, part, ssem.at[col, 0], rsem.at[side, sem], right[col]).wait_recv()
        g[core, col, pl.ds(first, count), rows] += buf[col, pl.ds(at, count), rows]

    def grams(s):
        for i in range(4):
            fetch(s, i).wait()

        w = w_ref[...]
        w3 = jnp.concatenate([w, w, w], axis=1)
        for i in range(8):
            t = xb[s % 2, i]
            tw = t * w3
            low = tdot(t[:, :256], tw[:, :256])
            high = tdot(t[:, 256:], tw[:, 128:])

            def put(half, col, row, value):
                g[half, col, s * 8 + i, pl.ds(row, value.shape[0]), :] = value

            pack(low, high, put)
            if i == 3:
                @pl.when(s == 0)
                def _():
                    pl.semaphore_wait(barrier, len(peers))

                for copy in halves(s, 0):
                    copy.start()
                for n in range(4, 8):
                    fetch(s, n).wait()

        for copy in halves(s, 1):
            copy.start()

    def summed(s):
        base = s * 8
        for copy in halves(s, 0) + halves(s, 1):
            copy.wait_recv()
        for col in range(3):
            g[core, col, pl.ds(base, 8), pl.ds(0, SIZE[col])] += pr[col, pl.ds(base, 8), pl.ds(0, SIZE[col])]
        xs, yh = order(s)

        @pl.when(xs == 0)
        def _():
            relay_right(0, base, 4, yh * 4, yh)
            relay_left(0, base + 4, 4, yh * 4, yh)

        @pl.when(xs == 1)
        def _():
            final_right(0, yh, base + 4, 4, yh * 8 + 4)

        @pl.when(xs == 2)
        def _():
            final_left(0, yh, base, 4, yh * 8)

        @pl.when(yh == 0)
        def _():
            relay_right(1, base, 2, xs * 2, 2 + xs)
            relay_left(1, base + 2, 2, xs * 2, 2 + xs)
            final_right(1, xs, base + 6, 2, xs * 4 + 2)

        @pl.when(yh == 1)
        def _():
            final_left(1, xs, base, 2, xs * 4)

        relay_right(2, base, 1, s, 6 + s)
        relay_left(2, base + 4, 1, s, 6 + s)
        final_right(2, yh * (1 + xs // 2), base + 5, 1, yh * 8 + 4 + xs)
        final_left(2, yh * (1 + xs // 2), base + 2, 1, yh * 8 + xs)

    def passed_x(s):
        base = s * 8
        xs, yh = order(s)

        @pl.when(xs == 1)
        def _():
            taken(rl, 0, 0, base, 4, yh * 4, yh)
            final_right(0, yh, base, 4, yh * 8)

        @pl.when(xs == 2)
        def _():
            taken(rr, 1, 0, base + 4, 4, yh * 4, yh)
            final_left(0, yh, base + 4, 4, yh * 8 + 4)

    def passed_yz(s):
        base = s * 8
        xs, yh = order(s)

        @pl.when(yh == 0)
        def _():
            taken(rl, 0, 1, base + 4, 2, xs * 2, 2 + xs)
            final_right(1, xs, base + 4, 2, xs * 4)

        @pl.when(yh == 1)
        def _():
            taken(rr, 1, 1, base + 2, 2, xs * 2, 2 + xs)
            final_left(1, xs, base + 2, 2, xs * 4 + 2)

        taken(rl, 0, 2, base + 1, 1, s, 6 + s)
        final_right(2, yh * (1 + xs // 2), base + 1, 1, yh * 8 + xs)
        taken(rr, 1, 2, base + 6, 1, s, 6 + s)
        final_left(2, yh * (1 + xs // 2), base + 6, 1, yh * 8 + 4 + xs)

    def step(s, carry):
        @pl.when(s < 7)
        def _():
            for i in range(8):
                fetch(s + 1, i).start()

        grams(s)

        @pl.when(s >= 1)
        def _():
            summed(s - 1)

        @pl.when(s == 5)
        def _():
            passed_x(2)

        @pl.when(s == 5)
        def _():
            passed_x(3)

        @pl.when(s == 7)
        def _():
            passed_x(4)
            passed_x(6)

        @pl.when(s >= LAG)
        def _():
            passed_yz(s - LAG)

        return carry

    lax.fori_loop(0, 8, step, 0)
    summed(7)

    def rest(s, carry):
        passed_yz(s)
        return carry

    lax.fori_loop(8 - LAG, 8, rest, 0)

    axis2, axis3 = (2, 0, 1), (1, 2, 0)
    hops = (far, right, left)

    def arrived(col, stage, first, count):
        for buf, side, to in ((fl, 0, left), (fr, 1, right)):
            whole = buf.at[col, pl.ds(first, count), pl.ds(0, SIZE[col])]
            remote(whole, whole, ssem.at[col, side], fsem.at[col, side, stage], to[col]).wait_recv()

    def complete(col, u, v):
        group, i, at = (
            ((3, v // 2), v % 2 * 4 + u, v * 4 + u),
            ((u, 1), 4 + v, u * 4 + v),
            ((v, u // 2), 3 + 4 * (u % 2), u * 4 + v),
        )[col]
        rows = pl.ds(0, SIZE[col])
        f1[col, u, v, rows] = g[core, col, GROUPS.index(group) * 8 + i, rows] + fl[col, at, rows] + fr[col, at, rows]

    def second(col, u, first, count):
        part = (pl.ds(first, count), pl.ds(0, SIZE[col]))
        remote(f1.at[(col, u) + part], q2.at[(col, u) + part], s2send.at[col], q2sem.at[col, u], hops[u][axis2[col]]).start()

    def along_x(u):
        arrived(1, u, u * 4, 4)
        for v in range(4):
            complete(1, u, v)
        if u < 3:
            second(1, u, 0, 4)

    def along_z(half):
        arrived(0, half, half * 8, 8)
        for u in range(4):
            for v in range(2 * half, 2 * half + 2):
                complete(0, u, v)
            if u < 3:
                second(0, u, 2 * half, 2)

    along_z(0)
    along_x(0)
    arrived(2, 0, 0, 8)
    for u in range(2):
        for v in range(4):
            complete(2, u, v)
        second(2, u, 0, 4)
    along_x(1)
    along_z(1)
    for k in range(2):
        arrived(2, 1 + k, 8, 4)
        for v in range(2 * k, 2 * k + 2):
            for u in range(2, 4):
                complete(2, u, v)
        second(2, 2, 2 * k, 2)
        along_x(2 + k)
    def third(col, k):
        rows = pl.ds(0, SIZE[col])
        return remote(f2.at[col, k, rows], f3.at[col, k, rows], s3send.at[col, k], s3sem.at[col, k], hops[k][axis3[col]])

    for col in range(3):
        rows = pl.ds(0, SIZE[col])
        for u in range(3):
            part = q2.at[col, u, :, rows]
            remote(part, part, s2send.at[col], q2sem.at[col, u], right[col]).wait_recv()
        f2[col, :, rows] = (f1[col, 3, :, rows] + q2[col, 0, :, rows]) + (q2[col, 1, :, rows] + q2[col, 2, :, rows])
        for k in range(3):
            third(col, k).start()
    for col in range(3):
        rows = pl.ds(0, SIZE[col])
        for k in range(3):
            third(col, k).wait_recv()
        h[core, pl.ds(START[col], SIZE[col])] = (f2[col, 3, rows] + f3[col, 0, rows]) + (f3[col, 1, rows] + f3[col, 2, rows])
    both = remote(h.at[core], h.at[core], hsem.at[0], hsem.at[1], partner)
    both.start()
    both.wait_recv()
    flat = jnp.concatenate([h[0], h[1]], axis=0)
    owner = (x * 16 + y * 4 + z) * 2 + core
    lane = lax.broadcasted_iota(jnp.int32, (1, 128), 1)
    exponent = jnp.where(lane == owner, dexp[...].astype(F32).reshape(1, 128), 0.0)
    scale = jnp.exp2(-jnp.sum(exponent, axis=1, keepdims=True))
    slot = z * 2 + core

    def emit(first, count, value):
        rows = pl.ds(first, count)
        own[rows] = value
        for k in range(8):
            to = device(x, base_y + (low_y + 1 - k // 4) % 2, (z + (2, 1, 3, 0)[k % 4]) % 4, low_y)
            copy = remote(own.at[rows], got.at[slot, rows], asem, bsem.at[slot], to)
            if k < 7:
                copy.start()
            else:
                pl.when(core != low_y)(copy.start)

        @pl.when(core == low_y)
        def _():
            got[slot, rows] = value

    whiten(flat, core == 0, scale, total, emit)

    for j in range(8):
        @pl.when(jnp.logical_or(core != low_y, slot != j))
        def _():
            remote(got.at[j], got.at[j], asem, bsem.at[j], partner).wait_recv()

    for col in range(3):
        for side in range(2):
            sent = g.at[core, col, pl.ds(0, 24), pl.ds(0, SIZE[col])]
            remote(sent, sent, ssem.at[col, side], fsem.at[col, side, 0], right[col]).wait_send()
        ahead = g.at[core, col, pl.ds(0, 12), pl.ds(0, SIZE[col])]
        remote(ahead, ahead, s2send.at[col], q2sem.at[col, 0], right[col]).wait_send()
        for k in range(3):
            third(col, k).wait_send()
    for col in range(3):
        every = g.at[1 - core, col, :, pl.ds(0, SIZE[col])]
        remote(every, every, dsend.at[col], drecv.at[0, 0, col], partner).wait_send()
    both.wait_send()
    seven = got.at[pl.ds(0, 7)]
    remote(seven, seven, asem, bsem.at[0], partner).wait_send()

    @pl.when(core != low_y)
    def _():
        remote(got.at[0], got.at[0], asem, bsem.at[0], partner).wait_send()


def unpack_kernel(packed, out_ref, full, sem):
    copies = []
    for j in range(8):
        full[j, 0:32, 0:64] = packed[j, 0:32, 0:64]
        full[j, 32:64, 0:64] = packed[j, 0:32, 64:128]
        full[j, 0:64, 64:192] = jnp.zeros((64, 128), F32)
        full[j, 64:128, 0:128] = packed[j, 32:96]
        full[j, 64:128, 128:192] = jnp.zeros((64, 64), F32)
        full[j, 128:192, 0:128] = packed[j, 96:160]
        full[j, 128:160, 128:192] = packed[j, 160:192, 0:64]
        full[j, 160:192, 128:192] = packed[j, 160:192, 64:128]
        copies.append(pltpu.make_async_copy(full.at[j], out_ref.at[j], sem.at[j]))
        copies[-1].start()
    for copy in copies:
        copy.wait()


def on_device(projected, weight_exp, damp_exp):
    total = projected.shape[0] * lax.axis_size('dp') * lax.axis_size('head')
    unit = (ROWS, 128)
    dma = pltpu.SemaphoreType.DMA
    packed = pl.pallas_call(
        functools.partial(whitening_kernel, total),
        out_shape=OUT((8, HD, 128), F32),
        in_specs=[pl.BlockSpec(memory_space=pl.ANY), pl.BlockSpec(memory_space=pl.ANY),
                  pl.BlockSpec(memory_space=pl.ANY)],
        out_specs=pl.BlockSpec(memory_space=pltpu.VMEM),
        scratch_shapes=[
            pltpu.VMEM((384,), jnp.int32), pltpu.VMEM((128,), jnp.int32), pltpu.VMEM((384, 128), jnp.bfloat16), dma((2,)),
            pltpu.VMEM((HD, 128), F32), dma, dma((8,)),
            pltpu.VMEM((2, 8, 384, 384), jnp.bfloat16),
            pltpu.VMEM((2, 3, 64) + unit, F32),
            pltpu.VMEM((3, 64) + unit, F32),
            pltpu.VMEM((3, 8) + unit, F32),
            pltpu.VMEM((3, 8) + unit, F32),
            pltpu.VMEM((3, 16) + unit, F32),
            pltpu.VMEM((3, 16) + unit, F32),
            pltpu.VMEM((3, 4, 4) + unit, F32),
            pltpu.VMEM((3, 3, 4) + unit, F32),
            pltpu.VMEM((3, 4) + unit, F32),
            pltpu.VMEM((3, 3) + unit, F32),
            pltpu.VMEM((2, 152, 128), F32),
            dma((2, 8)), dma((3,)), dma((8, 2, 3)), dma((2, 14)), dma((3, 2)), dma((3, 2, 4)),
            dma((3,)), dma((3, 3)), dma((3, 3)), dma((3, 3)), dma((2,)),
        ],
        compiler_params=pltpu.CompilerParams(collective_id=0, has_side_effects=True, vmem_limit_bytes=58 * 2**20),
        name="whitening",
    )(projected, weight_exp, damp_exp)
    return pl.pallas_call(
        unpack_kernel,
        out_shape=jax.ShapeDtypeStruct((8, HD, HD), F32),
        in_specs=[pl.BlockSpec(memory_space=pltpu.VMEM)],
        out_specs=pl.BlockSpec(memory_space=pl.ANY),
        scratch_shapes=[pltpu.VMEM((8, HD, HD), F32), dma((8,))],
        name="unpack",
    )(pltpu.with_memory_space_constraint(packed, pltpu.VMEM))


def solution(mesh):
    return jax.shard_map(
        on_device,
        mesh=mesh,
        in_specs=(P(("dp", "head"), None), P(("dp", "head")), P()),
        out_specs=P("head", None, None),
        check_vma=False,
    )
```
